128 devices in a mesh: row: 16 (over x, y), col: 8 (over z, core).
Axes of the slice: x: 4, y: 4, z: 4, core: 2. Of those that a mesh axis runs over, the one named last changes fastest.
Arguments:
- weights: int32 [8192, 8192], P('row', 'col'), may hold values from 1 to 64
Outputs:
- distances: int32 [8192, 8192], P('row', 'col')
The draws below stay inside these ranges and needn't reach their ends.
All inputs are finite; a program needn't handle non-finite values.
Results may differ from the reference program's by a relative error of at most 0.000001.
Values may be sent and summed in bfloat16 or wider, within the bound.
A program may use at most 64 MiB of HBM per device.

```python
import jax
import jax.numpy as jnp
from jax import lax

PIVOT = 128
STEPS = 4
VERTS = 8192
STRIDE = 2048


def set_ends(drawn, rng, low, top_value):
    shape = drawn.shape
    place = [jax.random.randint(jax.random.fold_in(rng, axis), (), 0, shape[axis]) for axis in range(len(shape))]
    drawn = drawn.at[tuple(place)].set(low)
    longest = shape.index(max(shape))
    place[longest] = (place[longest] + 1) % shape[longest]
    return drawn.at[tuple(place)].set(top_value)


def setup_inputs(seed: int = 0) -> dict:
    splits = jax.random.split(jax.random.key(seed), 2)
    weights = set_ends(jax.random.randint(splits[0], (VERTS, VERTS), 1, 65), jax.random.fold_in(splits[0], 1), 1, 64).astype(jnp.int32)
    return {"weights": weights}


def relax(vertex, dist):
    vertex = jnp.asarray(vertex).astype(jnp.int32)
    column = lax.dynamic_slice_in_dim(dist, vertex, 1, 1)
    across = lax.dynamic_slice_in_dim(dist, vertex, 1, 0)
    return jnp.minimum(dist, column + across)


def reference(weights):
    labels = jnp.arange(VERTS, dtype=jnp.int32)
    dist = jnp.where(labels[:, None] == labels[None, :], jnp.int32(0), weights).astype(jnp.int32)
    for step in range(STEPS):
        first = step * STRIDE
        dist = lax.fori_loop(first, first + PIVOT, relax, dist)
    return dist
```

```python
import jax
import jax.numpy as jnp
from jax import lax
from jax.experimental import pallas as pl
from jax.experimental.pallas import tpu as pltpu
from jax.sharding import PartitionSpec as P

F32 = jnp.float32
BF16 = jnp.bfloat16
MESH = pl.DeviceIdType.MESH
ALPHA = 60.25
BETA = 6.2
SHIFT = 0.984
STEP = 2.0**-BETA
B = 128
S = 4


def encode(values):
    t = values.astype(F32) - 1.0
    half = jnp.floor(t * 0.5)
    odd = (t - 2.0 * half) > 0.5
    return jnp.exp2(ALPHA - BETA * half), odd


def enc_right(values):
    e, odd = encode(values)
    return jnp.where(odd, e * STEP, e).astype(BF16), e.astype(BF16)


def enc_left(values):
    e, odd = encode(values)
    first = lax.broadcasted_iota(jnp.int32, values.shape, 1) < B // 2
    odd_floor = jnp.where(odd, e, 0.0)
    even = jnp.where(odd, 0.0, e)
    odd_ceil = odd_floor * STEP
    pairs = []
    for keep in (first, jnp.logical_not(first)):
        of, ev, oc = (jnp.where(keep, u, 0.0).astype(BF16) for u in (odd_floor, even, odd_ceil))
        pairs.append((jnp.concatenate([of, ev], 1), jnp.concatenate([ev, oc], 1)))
    return pairs


def dot(left, right):
    return jnp.dot(left, right, preferred_element_type=F32)


def level(total):
    x = (2 * ALPHA / BETA + SHIFT) - jnp.log2(total) * (1.0 / BETA)
    return jnp.floor(jnp.minimum(x, 200.0))


def decode(floors, ceils):
    low = level(floors)
    return low + jnp.minimum(level(ceils), low + 1.0) + 2.0


def min_plus(left, right, old):
    (f0, c0), (f1, c1) = left
    floors = jnp.maximum(dot(f0, right), dot(f1, right))
    ceils = jnp.maximum(dot(c0, right), dot(c1, right))
    return jnp.minimum(old, decode(floors, ceils))


def remote(src, dst, send, recv, where):
    return pltpu.make_async_remote_copy(
        src_ref=src, dst_ref=dst, send_sem=send, recv_sem=recv, device_id=where, device_id_type=MESH
    )


def kernel(
    w_hbm, o_ref, w, yp, yi, rr, y, enc_row, enc_r,
    w_sem, pp_send, pp_recv, yp_send, yp_recv, yi_send, yi_recv, fp_send, fi_send,
    rs_send, rs_recv, rg_send, rg_recv,
):
    row, col = lax.axis_index("row"), lax.axis_index("col")
    cx, cy = row // S, row % S
    cz, core = col // 2, col % 2

    barrier = pltpu.get_barrier_semaphore()
    for d in range(1, 16):
        pl.semaphore_signal(barrier, inc=1, device_id={"row": (row + d) % 16}, device_id_type=MESH)
    for d in range(1, 8):
        pl.semaphore_signal(barrier, inc=1, device_id={"col": (col + d) % 8}, device_id_type=MESH)

    loads = [
        pltpu.make_async_copy(w_hbm.at[pl.ds(i * B, B)], w.at[pl.ds(i * B, B)], w_sem.at[i])
        for i in range(S)
    ]
    for load in loads:
        load.start()
    loads[0].wait()

    @pl.when(cy == 0)
    def _():
        for q in range(S):
            rr[cx, q] = w[q * 32 : (q + 1) * 32, :].astype(BF16)

    @pl.when(jnp.logical_and(cy == 0, core == 0))
    def _():
        yp[cz, cx] = w[0:B, 0:B].astype(BF16)

    for load in loads[1:]:
        load.wait()

    @pl.when(core == 0)
    def _():
        yi[cz] = w[:, 0:B].astype(BF16)

    pl.semaphore_wait(barrier, 22)

    def pp_copy(s, d):
        return remote(yp.at[cz, s], yp.at[cz, s], pp_send.at[d], pp_recv.at[s], {"row": (row + d) % 16})

    def scatter_copy(q):
        return remote(rr.at[cx, q], rr.at[cx, q], rs_send.at[q], rs_recv, {"row": cx * S + q})

    def gather_copy(d):
        return remote(
            rr.at[cx, cy], rr.at[cx, cy], rg_send.at[d], rg_recv.at[row], {"row": (row + d) % 16}
        )

    @pl.when(core == 0)
    def _():
        @pl.when(cy == 0)
        def _():
            for d in range(1, 16):
                pp_copy(cx, d).start()

        def own(buf, send, recv):
            for d in range(1, S):
                remote(
                    buf.at[cz], buf.at[cz], send.at[d], recv.at[cz], {"col": (cz + d) % S * 2}
                ).start()
            remote(buf.at[cz], buf.at[cz], send.at[0], recv.at[cz], {"col": col + 1}).start()

        def forward(buf, send, recv, fwd):
            for d in range(1, S):
                other = (cz + d) % S
                remote(buf.at[other], buf.at[other], send.at[0], recv.at[other], {"col": col + 1}).wait_recv()
                remote(buf.at[other], buf.at[other], fwd.at[d], recv.at[other], {"col": col + 1}).start()

        own(yi, yi_send, yi_recv)
        for s in range(S):
            @pl.when(jnp.logical_not(jnp.logical_and(cy == 0, cx == s)))
            def _():
                pp_copy(s, 1).wait_recv()
        own(yp, yp_send, yp_recv)

        @pl.when(cy == 0)
        def _():
            for q in range(1, S):
                scatter_copy(q).start()

        forward(yi, yi_send, yi_recv, fi_send)
        forward(yp, yp_send, yp_recv, fp_send)

    @pl.when(core == 1)
    def _():
        remote(yp.at[cz], yp.at[cz], yp_send.at[0], yp_recv.at[cz], {"col": col - 1}).wait_recv()

        @pl.when(cy == 0)
        def _():
            for q in range(1, S):
                scatter_copy(q).start()

        for buf, send, recv in ((yi, yi_send, yi_recv), (yp, yp_send, yp_recv)):
            for d in range(S):
                other = (cz + d) % S
                if d == 0 and buf is yp:
                    continue
                remote(buf.at[other], buf.at[other], send.at[0], recv.at[other], {"col": col - 1}).wait_recv()

    @pl.when(cy != 0)
    def _():
        remote(rr.at[cx, cy], rr.at[cx, cy], rs_send.at[0], rs_recv, {"row": cx * S}).wait_recv()

    for d in range(1, 16):
        @pl.when(jnp.logical_or(cy == 0, (row + d) % 16 != cx * S))
        def _():
            gather_copy(d).start()

    for t in range(S):
        for s in range(S):
            y[t, s * B : (s + 1) * B, :] = yp[t, s].astype(F32)
        y[t, S * B :, :] = yi[t].astype(F32)

    def close(s, _):
        r0 = pl.multiple_of(s * B, B)

        def square(_, block):
            return min_plus(enc_left(block), jnp.concatenate(enc_right(block), 0), block)

        block = lax.fori_loop(0, 6, square, y[s, pl.ds(r0, B), :])
        y[s, pl.ds(r0, B), :] = block
        closed = enc_left(block)

        def panel(t, _):
            old = y[t, pl.ds(r0, B), :]
            new = min_plus(closed, jnp.concatenate(enc_right(old), 0), old)
            y[t, pl.ds(r0, B), :] = new
            ceil, floor = enc_right(new)
            enc_row[t, 0:B, :] = ceil
            enc_row[t, B : 2 * B, :] = floor
            return 0

        lax.fori_loop(0, S, panel, 0)

        def rows(i, _):
            i0 = pl.multiple_of(i * B, B)
            left = enc_left(y[s, pl.ds(i0, B), :])
            for t in range(S):
                y[t, pl.ds(i0, B), :] = min_plus(left, enc_row[t], y[t, pl.ds(i0, B), :])
            return 0

        lax.fori_loop(s + 1, 2 * S, rows, 0)
        return 0

    lax.fori_loop(0, S, close, 0)

    for d in range(1, 16):
        other = (row + d) % 16
        ox, oy = other // S, other % S

        @pl.when(jnp.logical_not(jnp.logical_and(cy == 0, ox == cx)))
        def _():
            remote(
                rr.at[ox, oy], rr.at[ox, oy], rg_send.at[0], rg_recv.at[other], {"row": other}
            ).wait_recv()

    for s in range(S):
        for q in range(S):
            ceil, floor = enc_right(rr[s, q])
            enc_r[s, q * 32 : (q + 1) * 32, :] = ceil
            enc_r[s, B + q * 32 : B + (q + 1) * 32, :] = floor

    def product(i, _):
        i0 = pl.multiple_of(i * B, B)
        y0 = pl.multiple_of(S * B + i * B, B)
        lefts = [enc_left(y[s, pl.ds(y0, B), :]) for s in range(S)]

        def columns(j, _):
            j0 = pl.multiple_of(j * 256, 256)
            floors = ceils = None
            for s in range(S):
                right = enc_r[s, :, pl.ds(j0, 256)]
                for left_floor, left_ceil in lefts[s]:
                    df, dc = dot(left_floor, right), dot(left_ceil, right)
                    floors = df if floors is None else jnp.maximum(floors, df)
                    ceils = dc if ceils is None else jnp.maximum(ceils, dc)
            found = decode(floors, ceils).astype(jnp.int32)
            old = w[pl.ds(i0, B), pl.ds(j0, 256)]
            lag = lax.broadcasted_iota(jnp.int32, old.shape, 1) - lax.broadcasted_iota(jnp.int32, old.shape, 0)
            old = jnp.where(lag == row * 512 + i0 - col * 1024 - j0, 0, old)
            o_ref[pl.ds(i0, B), pl.ds(j0, 256)] = jnp.minimum(old, found)
            return 0

        lax.fori_loop(0, 4, columns, 0)
        return 0

    lax.fori_loop(0, 4, product, 0)

    @pl.when(core == 0)
    def _():
        @pl.when(cy == 0)
        def _():
            for d in range(1, 16):
                pp_copy(cx, d).wait_send()

        for buf, send, fwd, recv in ((yi, yi_send, fi_send, yi_recv), (yp, yp_send, fp_send, yp_recv)):
            for d in range(S):
                remote(buf.at[cz], buf.at[cz], send.at[d], recv.at[cz], {"col": col + 1}).wait_send()
            for d in range(1, S):
                other = (cz + d) % S
                remote(buf.at[other], buf.at[other], fwd.at[d], recv.at[other], {"col": col + 1}).wait_send()

    @pl.when(cy == 0)
    def _():
        for q in range(1, S):
            scatter_copy(q).wait_send()

    for d in range(1, 16):
        @pl.when(jnp.logical_or(cy == 0, (row + d) % 16 != cx * S))
        def _():
            gather_copy(d).wait_send()


def per_device(weights):
    dma = pltpu.SemaphoreType.DMA
    return pl.pallas_call(
        kernel,
        out_shape=jax.ShapeDtypeStruct(weights.shape, jnp.int32),
        in_specs=[pl.BlockSpec(memory_space=pl.ANY)],
        out_specs=pl.BlockSpec(memory_space=pltpu.VMEM),
        scratch_shapes=[
            pltpu.VMEM((512, 1024), jnp.int32),
            pltpu.VMEM((S, S, B, B), BF16),
            pltpu.VMEM((S, 512, B), BF16),
            pltpu.VMEM((S, S, 32, 1024), BF16),
            pltpu.VMEM((S, 1024, B), F32),
            pltpu.VMEM((S, 2 * B, B), BF16),
            pltpu.VMEM((S, 2 * B, 1024), BF16),
            dma((S,)), dma((16,)), dma((S,)), dma((S,)), dma((S,)), dma((S,)), dma((S,)), dma((S,)), dma((S,)),
            dma((S,)), dma, dma((16,)), dma((16,)),
        ],
        compiler_params=pltpu.CompilerParams(
            collective_id=0, has_side_effects=True, vmem_limit_bytes=56 * 2**20
        ),
        name="paths",
    )(weights)


def solution(mesh):
    return jax.shard_map(
        per_device, mesh=mesh, in_specs=(P("row", "col"),), out_specs=P("row", "col"), check_vma=False
    )
```

```python
import jax
import jax.numpy as jnp
from jax import lax
from jax.experimental import pallas as pl
from jax.experimental.pallas import tpu as pltpu
from jax.sharding import PartitionSpec as P

F32 = jnp.float32
BF16 = jnp.bfloat16
MESH = pl.DeviceIdType.MESH
ALPHA = 60.25
BETA = 6.2
SHIFT = 0.984
STEP = 2.0**-BETA
B = 128
S = 4


def encode(values):
    t = values.astype(F32) - 1.0
    half = jnp.floor(t * 0.5)
    odd = (t - 2.0 * half) > 0.5
    return jnp.exp2(ALPHA - BETA * half), odd


def enc_right(values):
    e, odd = encode(values)
    return jnp.where(odd, e * STEP, e).astype(BF16), e.astype(BF16)


def enc_left(values):
    e, odd = encode(values)
    first = lax.broadcasted_iota(jnp.int32, values.shape, 1) < B // 2
    odd_floor = jnp.where(odd, e, 0.0)
    even = jnp.where(odd, 0.0, e)
    odd_ceil = odd_floor * STEP
    pairs = []
    for keep in (first, jnp.logical_not(first)):
        of, ev, oc = (jnp.where(keep, u, 0.0).astype(BF16) for u in (odd_floor, even, odd_ceil))
        pairs.append((jnp.concatenate([of, ev], 1), jnp.concatenate([ev, oc], 1)))
    return pairs


def dot(left, right):
    return jnp.dot(left, right, preferred_element_type=F32)


def level(total):
    x = (2 * ALPHA / BETA + SHIFT) - jnp.log2(total) * (1.0 / BETA)
    return jnp.floor(jnp.minimum(x, 200.0))


def decode(floors, ceils):
    low = level(floors)
    return low + jnp.minimum(level(ceils), low + 1.0) + 2.0


def min_plus(left, right, old):
    (f0, c0), (f1, c1) = left
    floors = jnp.maximum(dot(f0, right), dot(f1, right))
    ceils = jnp.maximum(dot(c0, right), dot(c1, right))
    return jnp.minimum(old, decode(floors, ceils))


def remote(src, dst, send, recv, where):
    return pltpu.make_async_remote_copy(
        src_ref=src, dst_ref=dst, send_sem=send, recv_sem=recv, device_id=where, device_id_type=MESH
    )


def gather_kernel(
    w_hbm, x_ref, r0, r1, wp, wr, wc, rs, yp, yi, y, enc_row,
    w_sem, p1_send, p1_recv, p2_send, p2_recv, pf_send, yi_send, yi_recv, fi_send,
    s0_send, s0_recv, s1_send, s1_recv, a0_send, a0_recv, a1_send, a1_recv, b0_send, b0_recv, b1_send, b1_recv,
):
    row, col = lax.axis_index("row"), lax.axis_index("col")
    cx, cy = row // S, row % S
    cz, core = col // 2, col % 2
    block_owner = jnp.logical_and(cy == 0, core == 0)

    def at_x(x):
        return {"row": x * S + cy}

    def at_y(v):
        return {"row": cx * S + v}

    def in_slab(d):
        other = (cx * S + cz + d) % 16
        ox, oz = other // S, other % S
        return ox, oz, {"row": ox * S + cy, "col": oz * 2 + core}

    partner = {"col": cz * 2 + (1 - core)}

    barrier = pltpu.get_barrier_semaphore()

    def greet(where):
        pl.semaphore_signal(barrier, inc=1, device_id=where, device_id_type=MESH)

    for d in range(1, S):
        greet(at_y((cy + d) % S))
    for d in range(1, 16):
        greet(in_slab(d)[2])
    greet(partner)

    load_block = pltpu.make_async_copy(w_hbm.at[pl.ds(0, B), pl.ds(0, B)], wp, w_sem.at[0])
    load_rows = pltpu.make_async_copy(w_hbm.at[pl.ds(0, B)], wr, w_sem.at[1])
    load_cols = pltpu.make_async_copy(w_hbm.at[:, pl.ds(0, B)], wc, w_sem.at[2])

    @pl.when(block_owner)
    def _():
        load_block.start()

    @pl.when(cy == 0)
    def _():
        load_rows.start()

    @pl.when(core == 0)
    def _():
        load_cols.start()

    @pl.when(block_owner)
    def _():
        load_block.wait()
        yp[cz, cx] = wp[...].astype(BF16)

    @pl.when(core == 0)
    def _():
        load_cols.wait()
        yi[cz] = wc[...].astype(BF16)

    @pl.when(cy == 0)
    def _():
        load_rows.wait()
        for q in range(S):
            for h in range(2):
                rs[q, h] = wr[q * 32 : (q + 1) * 32, h * 512 : (h + 1) * 512].astype(BF16)
        r0[0, cx] = wr[0:32, 0:512].astype(BF16)
        r1[cx, 0] = wr[0:32, 512:1024].astype(BF16)

    pl.semaphore_wait(barrier, 19)

    def block_y(d):
        return remote(yp.at[cz, cx], yp.at[cz, cx], p1_send.at[d], p1_recv, at_y((cy + d) % S))

    def block_out(d, where):
        return remote(yp.at[cz, cx], yp.at[cz, cx], p2_send.at[d], p2_recv.at[cz * S + cx], where)

    def block_in(ox, oz, send, where):
        return remote(yp.at[oz, ox], yp.at[oz, ox], send, p2_recv.at[oz * S + ox], where)

    def cols_out(d, where):
        return remote(yi.at[cz], yi.at[cz], yi_send.at[d], yi_recv.at[cz], where)

    def cols_in(oz, send):
        return remote(yi.at[oz], yi.at[oz], send, yi_recv.at[oz], partner)

    def scatter(q):
        return (
            remote(rs.at[q, 0], r0.at[q, cx], s0_send.at[q], s0_recv, at_y(q)),
            remote(rs.at[q, 1], r1.at[cx, q], s1_send.at[q], s1_recv, at_y(q)),
        )

    def stage_a(d, x, v):
        return (
            remote(r0.at[cy, x], r0.at[cy, x], a0_send.at[d], a0_recv.at[x], at_x((cx + d) % S)),
            remote(r1.at[cx, v], r1.at[cx, v], a1_send.at[d], a1_recv.at[v], at_y((cy + d) % S)),
        )

    def stage_b(d, x, v):
        return (
            remote(r0.at[v], r0.at[v], b0_send.at[d], b0_recv.at[v], at_y((cy + d) % S)),
            remote(r1.at[x], r1.at[x], b1_send.at[d], b1_recv.at[x], at_x((cx + d) % S)),
        )

    def start_scatter():
        @pl.when(cy == 0)
        def _():
            for q in range(1, S):
                for copy in scatter(q):
                    copy.start()

    def start_a():
        @pl.when(cy != 0)
        def _():
            for copy in scatter(cy):
                copy.wait_recv()

        for d in range(1, S):
            for copy in stage_a(d, cx, cy):
                copy.start()

    def start_b():
        for d in range(1, S):
            for copy in stage_a(d, (cx + d) % S, (cy + d) % S):
                copy.wait_recv()
        for d in range(1, S):
            for copy in stage_b(d, cx, cy):
                copy.start()

    @pl.when(core == 0)
    def _():
        @pl.when(cy == 0)
        def _():
            for d in range(1, S):
                block_y(d).start()

        for d in range(1, S):
            cols_out(d, {"col": (cz + d) % S * 2}).start()
        cols_out(0, partner).start()
        start_scatter()

        @pl.when(cy != 0)
        def _():
            block_y(0).wait_recv()

        for d in range(1, 16):
            block_out(d, in_slab(d)[2]).start()
        block_out(0, partner).start()
        start_a()
        for d in range(1, S):
            oz = (cz + d) % S
            cols_in(oz, yi_send.at[0]).wait_recv()
            cols_in(oz, fi_send.at[d]).start()
        for d in range(1, 16):
            ox, oz, _ = in_slab(d)
            block_in(ox, oz, p2_send.at[0], partner).wait_recv()
            block_in(ox, oz, pf_send.at[d], partner).start()

    @pl.when(core == 1)
    def _():
        start_scatter()
        start_a()
        for oz in range(S):
            cols_in(oz, yi_send.at[0]).wait_recv()
        for d in range(16):
            ox, oz, _ = in_slab(d)
            block_in(ox, oz, p2_send.at[0], partner).wait_recv()

    start_b()

    for t in range(S):
        lanes = slice(t % 2 * B, (t % 2 + 1) * B)
        for s in range(S):
            y[t // 2, s * B : (s + 1) * B, lanes] = yp[t, s].astype(F32)
        y[t // 2, S * B :, lanes] = yi[t].astype(F32)

    def rows_of(i):
        return pl.ds(pl.multiple_of(i * B, B), B)

    def column(s, i):
        return y.at[s // 2, rows_of(i), pl.ds(pl.multiple_of(s % 2 * B, B), B)]

    def square(block):
        return min_plus(enc_left(block), jnp.concatenate(enc_right(block), 0), block)

    def update(s, i):
        left = enc_left(column(s, i)[...])
        for u in range(2):
            y[u, rows_of(i), :] = min_plus(left, enc_row[u], y[u, rows_of(i), :])

    def panel(s, block):
        column(s, s)[...] = block
        closed = enc_left(block)
        for u in range(2):
            old = y[u, rows_of(s), :]
            new = min_plus(closed, jnp.concatenate(enc_right(old), 0), old)
            y[u, rows_of(s), :] = new
            ceil, floor = enc_right(new)
            enc_row[u, 0:B, :] = ceil
            enc_row[u, B : 2 * B, :] = floor

    def close(s, block):
        panel(s, block)
        lax.fori_loop(s + 1, S, lambda i, _: update(s, i), None)

        def both(i, block):
            update(s, S + i)
            return square(block)

        block = lax.fori_loop(0, S, both, column(s + 1, s + 1)[...])
        return lax.fori_loop(0, 2, lambda _, block: square(block), block)

    block = lax.fori_loop(0, 6, lambda _, block: square(block), column(0, 0)[...])
    block = lax.fori_loop(0, S - 1, close, block)
    panel(S - 1, block)
    lax.fori_loop(S, 2 * S, lambda i, _: update(S - 1, i), None)
    for t in range(S):
        x_ref[t] = y[t // 2, S * B :, t % 2 * B : (t % 2 + 1) * B].astype(BF16)

    for d in range(1, S):
      for copy in stage_b(d, (cx + d) % S, (cy + d) % S):
          copy.wait_recv()

    @pl.when(core == 0)
    def _():
        @pl.when(cy == 0)
        def _():
            for d in range(1, S):
                block_y(d).wait_send()

        for d in range(16):
            block_out(d, partner).wait_send()
        for d in range(S):
            cols_out(d, partner).wait_send()
        for d in range(1, S):
            cols_in((cz + d) % S, fi_send.at[d]).wait_send()
        for d in range(1, 16):
            ox, oz, _ = in_slab(d)
            block_in(ox, oz, pf_send.at[d], partner).wait_send()

    @pl.when(cy == 0)
    def _():
      for q in range(1, S):
          for copy in scatter(q):
              copy.wait_send()

    for d in range(1, S):
      for copy in stage_a(d, cx, cy):
          copy.wait_send()
    for d in range(1, S):
      for copy in stage_b(d, cx, cy):
          copy.wait_send()


def product_kernel(w_ref, x_ref, r0, r1, o_ref, enc_r):
    i = pl.program_id(0)
    row, col = lax.axis_index("row"), lax.axis_index("col")

    @pl.when(i == 0)
    def _():
        def encode_strip(s, _):
            for q in range(S):
                for h, part in ((0, r0[q, s]), (1, r1[s, q])):
                    ceil, floor = enc_right(part)
                    enc_r[s, q * 32 : (q + 1) * 32, h * 512 : (h + 1) * 512] = ceil
                    enc_r[s, B + q * 32 : B + (q + 1) * 32, h * 512 : (h + 1) * 512] = floor
            return 0

        lax.fori_loop(0, S, encode_strip, 0)

    lefts = [enc_left(x_ref[s]) for s in range(S)]

    def columns(j, _):
        j0 = pl.multiple_of(j * 256, 256)
        floors = ceils = None
        for s in range(S):
            right = enc_r[s, :, pl.ds(j0, 256)]
            for left_floor, left_ceil in lefts[s]:
                df, dc = dot(left_floor, right), dot(left_ceil, right)
                floors = df if floors is None else jnp.maximum(floors, df)
                ceils = dc if ceils is None else jnp.maximum(ceils, dc)
        found = decode(floors, ceils).astype(jnp.int32)
        old = w_ref[:, pl.ds(j0, 256)]
        lag = lax.broadcasted_iota(jnp.int32, old.shape, 1) - lax.broadcasted_iota(jnp.int32, old.shape, 0)
        old = jnp.where(lag == row * 512 + i * B - col * 1024 - j0, 0, old)
        o_ref[:, pl.ds(j0, 256)] = jnp.minimum(old, found)
        return 0

    lax.fori_loop(0, 4, columns, 0)


def per_device(weights):
    dma = pltpu.SemaphoreType.DMA
    vmem = pl.BlockSpec(memory_space=pltpu.VMEM)
    rows, cols = weights.shape
    closed, r0, r1 = pl.pallas_call(
        gather_kernel,
        out_shape=(
            jax.ShapeDtypeStruct((S, rows, B), BF16),
            jax.ShapeDtypeStruct((S, S, 32, 512), BF16),
            jax.ShapeDtypeStruct((S, S, 32, 512), BF16),
        ),
        in_specs=[pl.BlockSpec(memory_space=pltpu.HBM)],
        out_specs=(vmem, vmem, vmem),
        scratch_shapes=[
            pltpu.VMEM((B, B), jnp.int32),
            pltpu.VMEM((B, cols), jnp.int32),
            pltpu.VMEM((rows, B), jnp.int32),
            pltpu.VMEM((S, 2, 32, 512), BF16),
            pltpu.VMEM((S, S, B, B), BF16),
            pltpu.VMEM((S, rows, B), BF16),
            pltpu.VMEM((2, 1024, 2 * B), F32),
            pltpu.VMEM((2, 2 * B, 2 * B), BF16),
            dma((3,)), dma((S,)), dma, dma((16,)), dma((16,)), dma((16,)), dma((S,)), dma((S,)), dma((S,)),
            dma((S,)), dma, dma((S,)), dma,
            dma((S,)), dma((S,)), dma((S,)), dma((S,)), dma((S,)), dma((S,)), dma((S,)), dma((S,)),
        ],
        compiler_params=pltpu.CompilerParams(
            collective_id=0, has_side_effects=True, vmem_limit_bytes=24 * 2**20
        ),
        name="gather",
    )(weights)
    return pl.pallas_call(
        product_kernel,
        grid=(S,),
        out_shape=jax.ShapeDtypeStruct(weights.shape, jnp.int32),
        in_specs=[
            pl.BlockSpec((B, cols), lambda i: (i, 0)),
            pl.BlockSpec((S, B, B), lambda i: (0, i, 0)),
            vmem,
            vmem,
        ],
        out_specs=pl.BlockSpec((B, cols), lambda i: (i, 0)),
        scratch_shapes=[pltpu.VMEM((S, 2 * B, cols), BF16)],
        compiler_params=pltpu.CompilerParams(vmem_limit_bytes=24 * 2**20),
        name="product",
    )(weights, closed, r0, r1)


def solution(mesh):
    return jax.shard_map(
        per_device, mesh=mesh, in_specs=(P("row", "col"),), out_specs=P("row", "col"), check_vma=False
    )
```

```python
import math

import jax
import jax.numpy as jnp
from jax import lax
from jax.experimental import pallas as pl
from jax.experimental.pallas import tpu as pltpu
from jax.sharding import PartitionSpec as P

F32 = jnp.float32
BF16 = jnp.bfloat16
MESH = pl.DeviceIdType.MESH
ALPHA = 60.25
BETA = 6.2
SHIFT = 0.984
STEP = 2.0**-BETA
B = 128
S = 4


LOG = 1.0 / (BETA * math.log(2.0))
FLOOR = 2 * ALPHA / BETA + SHIFT


def encode(t):
    u = t * 0.5
    half = jnp.floor(u)
    return jnp.exp2(half * -BETA + ALPHA), u > half


def enc_right(t):
    e, odd = encode(t)
    return jnp.where(odd, e * STEP, e).astype(BF16), e.astype(BF16)


def split_left(t):
    e, odd = encode(t)
    odd_floor = jnp.where(odd, e, 0.0)
    return tuple(u.astype(BF16) for u in (odd_floor, jnp.where(odd, 0.0, e), odd_floor * STEP))


def enc_left(t):
    first = jnp.where(lax.broadcasted_iota(jnp.int32, t.shape, 1) < B // 2, 1.0, 0.0)
    pairs = []
    parts = split_left(t)
    for keep in (first.astype(BF16), (1.0 - first).astype(BF16)):
        of, ev, oc = (u * keep for u in parts)
        pairs.append((jnp.concatenate([of, ev], 1), jnp.concatenate([ev, oc], 1)))
    return pairs


def dot(left, right):
    return jnp.dot(left, right, preferred_element_type=F32)


def decode(floors, ceils, bias):
    low = jnp.floor(FLOOR - jnp.log(floors) * LOG)
    high = jnp.floor(FLOOR + bias - jnp.log(ceils) * LOG)
    return low + jnp.minimum(high, low + (1.0 + bias))


def min_plus(left, right, old):
    (f0, c0), (f1, c1) = left
    floors = jnp.maximum(dot(f0, right), dot(f1, right))
    ceils = jnp.maximum(dot(c0, right), dot(c1, right))
    return jnp.minimum(old, decode(floors, ceils, 1.0))


def min_plus_block(block):
    of, ev, oc = split_left(block)
    ceil, floor = enc_right(block)
    none = jnp.zeros((B // 2, B), BF16)
    first = jnp.concatenate([ceil[: B // 2], none, floor[: B // 2], none], 0)
    second = jnp.concatenate([none, ceil[B // 2 :], none, floor[B // 2 :]], 0)
    right = jnp.concatenate([first, second], 1)
    floors = dot(jnp.concatenate([of, ev], 1), right)
    ceils = dot(jnp.concatenate([ev, oc], 1), right)
    floors = jnp.maximum(floors[:, :B], floors[:, B:])
    ceils = jnp.maximum(ceils[:, :B], ceils[:, B:])
    return jnp.minimum(block, decode(floors, ceils, 1.0))


def remote(src, dst, send, recv, where):
    return pltpu.make_async_remote_copy(
        src_ref=src, dst_ref=dst, send_sem=send, recv_sem=recv, device_id=where, device_id_type=MESH
    )


def gather_kernel(
    w, x_ref, r0, r1, rs, yp, yi, y, enc_row,
    p1_send, p1_recv, p2_send, p2_recv, pf_send, yi_send, yi_recv, fi_send,
    s0_send, s0_recv, s1_send, s1_recv, a0_send, a0_recv, a1_send, a1_recv, b0_send, b0_recv, b1_send, b1_recv,
):
    row, col = lax.axis_index("row"), lax.axis_index("col")
    cx, cy = row // S, row % S
    cz, core = col // 2, col % 2
    block_owner = jnp.logical_and(cy == 0, core == 0)

    def at_x(x):
        return {"row": x * S + cy}

    def at_y(v):
        return {"row": cx * S + v}

    def in_slab(d):
        other = (cx * S + cz + d) % 16
        ox, oz = other // S, other % S
        return ox, oz, {"row": ox * S + cy, "col": oz * 2 + core}

    partner = {"col": cz * 2 + (1 - core)}

    barrier = pltpu.get_barrier_semaphore()

    def greet(where):
        pl.semaphore_signal(barrier, inc=1, device_id=where, device_id_type=MESH)

    for d in range(1, S):
        greet(at_y((cy + d) % S))
    for d in range(1, 16):
        greet(in_slab(d)[2])
    greet(partner)

    @pl.when(block_owner)
    def _():
        yp[cz, cx] = w[0:B, 0:B].astype(BF16)

    @pl.when(core == 0)
    def _():
        yi[cz] = w[:, 0:B].astype(BF16)

    @pl.when(cy == 0)
    def _():
        for q in range(S):
            for h in range(2):
                rs[q, h] = w[q * 32 : (q + 1) * 32, h * 512 : (h + 1) * 512].astype(BF16)
        r0[0, cx] = w[0:32, 0:512].astype(BF16)
        r1[cx, 0] = w[0:32, 512:1024].astype(BF16)

    pl.semaphore_wait(barrier, 19)

    def block_y(d):
        return remote(yp.at[cz, cx], yp.at[cz, cx], p1_send.at[d], p1_recv, at_y((cy + d) % S))

    def block_out(d, where):
        return remote(yp.at[cz, cx], yp.at[cz, cx], p2_send.at[d], p2_recv.at[cz * S + cx], where)

    def block_in(ox, oz, send, where):
        return remote(yp.at[oz, ox], yp.at[oz, ox], send, p2_recv.at[oz * S + ox], where)

    def cols_out(d, where):
        return remote(yi.at[cz], yi.at[cz], yi_send.at[d], yi_recv.at[cz], where)

    def cols_in(oz, send):
        return remote(yi.at[oz], yi.at[oz], send, yi_recv.at[oz], partner)

    def scatter(q):
        return (
            remote(rs.at[q, 0], r0.at[q, cx], s0_send.at[q], s0_recv, at_y(q)),
            remote(rs.at[q, 1], r1.at[cx, q], s1_send.at[q], s1_recv, at_y(q)),
        )

    def stage_a(d, x, v):
        return (
            remote(r0.at[cy, x], r0.at[cy, x], a0_send.at[d], a0_recv.at[x], at_x((cx + d) % S)),
            remote(r1.at[cx, v], r1.at[cx, v], a1_send.at[d], a1_recv.at[v], at_y((cy + d) % S)),
        )

    def stage_b(d, x, v):
        return (
            remote(r0.at[v], r0.at[v], b0_send.at[d], b0_recv.at[v], at_y((cy + d) % S)),
            remote(r1.at[x], r1.at[x], b1_send.at[d], b1_recv.at[x], at_x((cx + d) % S)),
        )

    def start_scatter():
        @pl.when(cy == 0)
        def _():
            for q in range(1, S):
                for copy in scatter(q):
                    copy.start()

    def start_a():
        @pl.when(cy != 0)
        def _():
            for copy in scatter(cy):
                copy.wait_recv()

        for d in range(1, S):
            for copy in stage_a(d, cx, cy):
                copy.start()

    def start_b():
        for d in range(1, S):
            for copy in stage_a(d, (cx + d) % S, (cy + d) % S):
                copy.wait_recv()
        for d in range(1, S):
            for copy in stage_b(d, cx, cy):
                copy.start()

    @pl.when(block_owner)
    def _():
        for d in range(1, S):
            block_y(d).start()

    @pl.when(core == 0)
    def _():
        for d in range(1, S):
            cols_out(d, {"col": (cz + d) % S * 2}).start()
        cols_out(0, partner).start()
        start_scatter()

        @pl.when(cy != 0)
        def _():
            block_y(0).wait_recv()

        for d in range(1, 16):
            block_out(d, in_slab(d)[2]).start()
        block_out(0, partner).start()
        start_a()
        for d in range(1, S):
            oz = (cz + d) % S
            cols_in(oz, yi_send.at[0]).wait_recv()
            cols_in(oz, fi_send.at[d]).start()

    @pl.when(core == 1)
    def _():
        start_scatter()
        start_a()
        for oz in range(S):
            cols_in(oz, yi_send.at[0]).wait_recv()
        block_in(cx, cz, p2_send.at[0], partner).wait_recv()

    here = cx * S + cz

    def take(d):
        ox, oz, _ = in_slab(d)
        block_in(ox, oz, p2_send.at[0], partner).wait_recv()

        @pl.when(core == 0)
        def _():
            block_in(ox, oz, pf_send.at[d], partner).start()

    def take_other(d):
        @pl.when((here + d) % 16 != 0)
        def _():
            take(d)

    def rows_of(i):
        return pl.ds(i * B, B)

    def column(s, i):
        return y.at[s // 2, rows_of(i), pl.ds(s % 2 * B, B)]

    def update(s, i, which=(0, 1)):
        left = enc_left(column(s, i)[...])
        for u in which:
            y[u, rows_of(i), :] = min_plus(left, enc_row[s % 2, u], y[u, rows_of(i), :])

    def panel(s, block):
        column(s, s)[...] = block
        closed = enc_left(block)
        for u in range(2):
            old = y[u, rows_of(s), :]
            new = min_plus(closed, jnp.concatenate(enc_right(old), 0), old)
            y[u, rows_of(s), :] = new
            ceil, floor = enc_right(new)
            enc_row[s % 2, u, 0:B, :] = ceil
            enc_row[s % 2, u, B : 2 * B, :] = floor

    @pl.when(here != 0)
    def _():
        take((16 - here) % 16)

    def square_and_take(i, block):
        block = min_plus_block(block)
        for d in range(3):
            take_other(1 + 3 * i + d)
        return block

    block = lax.fori_loop(0, 5, square_and_take, yp[0, 0].astype(F32) - 1.0)
    start_b()
    block = min_plus_block(block)

    for t in range(S):
        lanes = slice(t % 2 * B, (t % 2 + 1) * B)
        for s in range(S):
            y[t // 2, s * B : (s + 1) * B, lanes] = yp[t, s].astype(F32) - 1.0
        y[t // 2, S * B :, lanes] = yi[t].astype(F32) - 1.0

    for s in range(S - 1):
        panel(s, block)
        near = (s + 1) // 2
        update(s, s + 1, (near,))
        block = column(s + 1, s + 1)[...]
        rest = [(s + 1, (1 - near,))] + [(i, (0, 1)) for i in range(s + 2, 2 * S)]
        done = 0
        for q in range(6):
            block = min_plus_block(block)
            until = -(-len(rest) * (q + 1) // 6)
            for i, which in rest[done:until]:
                update(s, i, which)
            done = until
    panel(S - 1, block)
    for i in range(S, 2 * S):
        update(S - 1, i)
    for t in range(S):
        x_ref[t] = y[t // 2, S * B :, t % 2 * B : (t % 2 + 1) * B].astype(BF16)

    for d in range(1, S):
        for copy in stage_b(d, (cx + d) % S, (cy + d) % S):
            copy.wait_recv()

    @pl.when(core == 0)
    def _():
        @pl.when(cy == 0)
        def _():
            for d in range(1, S):
                block_y(d).wait_send()

        for d in range(16):
            block_out(d, partner).wait_send()
        for d in range(S):
            cols_out(d, partner).wait_send()
        for d in range(1, S):
            cols_in((cz + d) % S, fi_send.at[d]).wait_send()
        for d in range(1, 16):
            ox, oz, _ = in_slab(d)
            block_in(ox, oz, pf_send.at[d], partner).wait_send()

    @pl.when(cy == 0)
    def _():
      for q in range(1, S):
          for copy in scatter(q):
              copy.wait_send()

    for d in range(1, S):
      for copy in stage_a(d, cx, cy):
          copy.wait_send()
    for d in range(1, S):
      for copy in stage_b(d, cx, cy):
          copy.wait_send()


def product_kernel(w, x_ref, r0, r1, o_hbm, o, enc_r, o_sem):
    row, col = lax.axis_index("row"), lax.axis_index("col")
    wide = 2 * B
    parts = [pl.ds(j * wide, wide) for j in range(w.shape[1] // wide)]
    stores = [pltpu.make_async_copy(o.at[:, p], o_hbm.at[:, p], o_sem.at[j]) for j, p in enumerate(parts)]

    def encode_strip(s, _):
        for q in range(S):
            for h, part in ((0, r0[q, s]), (1, r1[s, q])):
                ceil, floor = enc_right(part.astype(F32) - 1.0)
                enc_r[s, q * 32 : (q + 1) * 32, h * 512 : (h + 1) * 512] = ceil
                enc_r[s, B + q * 32 : B + (q + 1) * 32, h * 512 : (h + 1) * 512] = floor
        return 0

    lax.fori_loop(0, S, encode_strip, 0)
    lefts = [enc_left(x_ref[s].astype(F32)) for s in range(S)]
    for j, p in enumerate(parts):
        floors = ceils = None
        for s in range(S):
            right = enc_r[s, :, p]
            for left_floor, left_ceil in lefts[s]:
                df, dc = dot(left_floor, right), dot(left_ceil, right)
                floors = df if floors is None else jnp.maximum(floors, df)
                ceils = dc if ceils is None else jnp.maximum(ceils, dc)
        old = w[:, p]
        new = jnp.minimum(old.astype(F32), decode(floors, ceils, 2.0)).astype(jnp.int32)
        lag = lax.broadcasted_iota(jnp.int32, old.shape, 1) - lax.broadcasted_iota(jnp.int32, old.shape, 0)
        o[:, p] = jnp.where(lag == row * w.shape[0] - col * w.shape[1] - j * wide, 0, new)
        stores[j].start()
    for store in stores:
        store.wait()


def per_device(weights):
    dma = pltpu.SemaphoreType.DMA
    vmem = pl.BlockSpec(memory_space=pltpu.VMEM)
    rows, cols = weights.shape
    closed, r0, r1 = pl.pallas_call(
        gather_kernel,
        out_shape=(
            jax.ShapeDtypeStruct((S, rows, B), BF16),
            jax.ShapeDtypeStruct((S, S, 32, 512), BF16),
            jax.ShapeDtypeStruct((S, S, 32, 512), BF16),
        ),
        in_specs=[vmem],
        out_specs=(vmem, vmem, vmem),
        scratch_shapes=[
            pltpu.VMEM((S, 2, 32, 512), BF16),
            pltpu.VMEM((S, S, B, B), BF16),
            pltpu.VMEM((S, rows, B), BF16),
            pltpu.VMEM((2, 1024, 2 * B), F32),
            pltpu.VMEM((2, 2, 2 * B, 2 * B), BF16),
            dma((S,)), dma, dma((16,)), dma((16,)), dma((16,)), dma((S,)), dma((S,)), dma((S,)),
            dma((S,)), dma, dma((S,)), dma,
            dma((S,)), dma((S,)), dma((S,)), dma((S,)), dma((S,)), dma((S,)), dma((S,)), dma((S,)),
        ],
        compiler_params=pltpu.CompilerParams(
            collective_id=0, has_side_effects=True, vmem_limit_bytes=24 * 2**20
        ),
        name="gather",
    )(weights)
    return pl.pallas_call(
        product_kernel,
        out_shape=jax.ShapeDtypeStruct(weights.shape, jnp.int32),
        in_specs=[vmem] * 4,
        out_specs=pl.BlockSpec(memory_space=pltpu.HBM),
        scratch_shapes=[
            pltpu.VMEM((rows, cols), jnp.int32),
            pltpu.VMEM((S, 2 * B, cols), BF16),
            dma((4,)),
        ],
        compiler_params=pltpu.CompilerParams(vmem_limit_bytes=32 * 2**20),
        name="product",
    )(weights, closed, r0, r1)


def solution(mesh):
    return jax.shard_map(
        per_device, mesh=mesh, in_specs=(P("row", "col"),), out_specs=P("row", "col"), check_vma=False
    )
```

```python
import math

import jax
import jax.numpy as jnp
from jax import lax
from jax.experimental import pallas as pl
from jax.experimental.pallas import tpu as pltpu
from jax.sharding import PartitionSpec as P

F32 = jnp.float32
BF16 = jnp.bfloat16
MESH = pl.DeviceIdType.MESH
ALPHA = 60.25
BETA = 6.2
SHIFT = 0.984
STEP = 2.0**-BETA
B = 128
S = 4


LOG = 1.0 / (BETA * math.log(2.0))
FLOOR = 2 * ALPHA / BETA + SHIFT


def encode(t):
    u = t * 0.5
    half = jnp.floor(u)
    return jnp.exp2(half * -BETA + ALPHA), u > half


def enc_right(t):
    e, odd = encode(t)
    return jnp.where(odd, e * STEP, e).astype(BF16), e.astype(BF16)


def split_left(t):
    e, odd = encode(t)
    odd_floor = jnp.where(odd, e, 0.0)
    return tuple(u.astype(BF16) for u in (odd_floor, jnp.where(odd, 0.0, e), odd_floor * STEP))


def enc_left(t):
    first = jnp.where(lax.broadcasted_iota(jnp.int32, t.shape, 1) < B // 2, 1.0, 0.0)
    pairs = []
    parts = split_left(t)
    for keep in (first.astype(BF16), (1.0 - first).astype(BF16)):
        of, ev, oc = (u * keep for u in parts)
        pairs.append((jnp.concatenate([of, ev], 1), jnp.concatenate([ev, oc], 1)))
    return pairs


def dot(left, right):
    return jnp.dot(left, right, preferred_element_type=F32)


def decode(floors, ceils, bias):
    low = jnp.floor(FLOOR - jnp.log(floors) * LOG)
    high = jnp.floor(FLOOR + bias - jnp.log(ceils) * LOG)
    return low + jnp.minimum(high, low + (1.0 + bias))


def min_plus(left, right, old):
    (f0, c0), (f1, c1) = left
    floors = jnp.maximum(dot(f0, right), dot(f1, right))
    ceils = jnp.maximum(dot(c0, right), dot(c1, right))
    return jnp.minimum(old, decode(floors, ceils, 1.0))


def min_plus_block(block):
    of, ev, oc = split_left(block)
    ceil, floor = enc_right(block)
    none = jnp.zeros((B // 2, B), BF16)
    first = jnp.concatenate([ceil[: B // 2], none, floor[: B // 2], none], 0)
    second = jnp.concatenate([none, ceil[B // 2 :], none, floor[B // 2 :]], 0)
    right = jnp.concatenate([first, second], 1)
    floors = dot(jnp.concatenate([of, ev], 1), right)
    ceils = dot(jnp.concatenate([ev, oc], 1), right)
    floors = jnp.maximum(floors[:, :B], floors[:, B:])
    ceils = jnp.maximum(ceils[:, :B], ceils[:, B:])
    return jnp.minimum(block, decode(floors, ceils, 1.0))


def remote(src, dst, send, recv, where):
    return pltpu.make_async_remote_copy(
        src_ref=src, dst_ref=dst, send_sem=send, recv_sem=recv, device_id=where, device_id_type=MESH
    )


def gather_kernel(
    w_hbm, x_ref, r0, r1, wp, wr, wc, rs, yp, yi, y, enc_row,
    w_sem, p1_send, p1_recv, p2_send, p2_recv, pf_send, yi_send, yi_recv, fi_send,
    s0_send, s0_recv, s1_send, s1_recv, a0_send, a0_recv, a1_send, a1_recv, b0_send, b0_recv, b1_send, b1_recv,
):
    row, col = lax.axis_index("row"), lax.axis_index("col")
    cx, cy = row // S, row % S
    cz, core = col // 2, col % 2
    block_owner = jnp.logical_and(cy == 0, core == 0)

    def at_x(x):
        return {"row": x * S + cy}

    def at_y(v):
        return {"row": cx * S + v}

    def in_slab(d):
        other = (cx * S + cz + d) % 16
        ox, oz = other // S, other % S
        return ox, oz, {"row": ox * S + cy, "col": oz * 2 + core}

    partner = {"col": cz * 2 + (1 - core)}

    barrier = pltpu.get_barrier_semaphore()

    def greet(where):
        pl.semaphore_signal(barrier, inc=1, device_id=where, device_id_type=MESH)

    for d in range(1, S):
        greet(at_y((cy + d) % S))
    for d in range(1, 16):
        greet(in_slab(d)[2])
    greet(partner)

    load_block = pltpu.make_async_copy(w_hbm.at[pl.ds(0, B), pl.ds(0, B)], wp, w_sem.at[0])
    load_rows = pltpu.make_async_copy(w_hbm.at[pl.ds(0, B)], wr, w_sem.at[1])
    load_cols = pltpu.make_async_copy(w_hbm.at[:, pl.ds(0, B)], wc, w_sem.at[2])

    @pl.when(block_owner)
    def _():
        load_block.start()

    @pl.when(cy == 0)
    def _():
        load_rows.start()

    @pl.when(core == 0)
    def _():
        load_cols.start()

    @pl.when(block_owner)
    def _():
        load_block.wait()
        yp[cz, cx] = wp[...].astype(BF16)

    pl.semaphore_wait(barrier, 19)

    def block_y(d):
        return remote(yp.at[cz, cx], yp.at[cz, cx], p1_send.at[d], p1_recv, at_y((cy + d) % S))

    def block_out(d, where):
        return remote(yp.at[cz, cx], yp.at[cz, cx], p2_send.at[d], p2_recv.at[cz * S + cx], where)

    def block_in(ox, oz, send, where):
        return remote(yp.at[oz, ox], yp.at[oz, ox], send, p2_recv.at[oz * S + ox], where)

    def cols_out(d, where):
        return remote(yi.at[cz], yi.at[cz], yi_send.at[d], yi_recv.at[cz], where)

    def cols_in(oz, send):
        return remote(yi.at[oz], yi.at[oz], send, yi_recv.at[oz], partner)

    def scatter(q):
        return (
            remote(rs.at[q, 0], r0.at[q, cx], s0_send.at[q], s0_recv, at_y(q)),
            remote(rs.at[q, 1], r1.at[cx, q], s1_send.at[q], s1_recv, at_y(q)),
        )

    def stage_a(d, x, v):
        return (
            remote(r0.at[cy, x], r0.at[cy, x], a0_send.at[d], a0_recv.at[x], at_x((cx + d) % S)),
            remote(r1.at[cx, v], r1.at[cx, v], a1_send.at[d], a1_recv.at[v], at_y((cy + d) % S)),
        )

    def stage_b(d, x, v):
        return (
            remote(r0.at[v], r0.at[v], b0_send.at[d], b0_recv.at[v], at_y((cy + d) % S)),
            remote(r1.at[x], r1.at[x], b1_send.at[d], b1_recv.at[x], at_x((cx + d) % S)),
        )

    def start_scatter():
        @pl.when(cy == 0)
        def _():
            for q in range(1, S):
                for copy in scatter(q):
                    copy.start()

    def start_a():
        @pl.when(cy != 0)
        def _():
            for copy in scatter(cy):
                copy.wait_recv()

        for d in range(1, S):
            for copy in stage_a(d, cx, cy):
                copy.start()

    def start_b():
        for d in range(1, S):
            for copy in stage_a(d, (cx + d) % S, (cy + d) % S):
                copy.wait_recv()
        for d in range(1, S):
            for copy in stage_b(d, cx, cy):
                copy.start()

    @pl.when(block_owner)
    def _():
        for d in range(1, S):
            block_y(d).start()

    @pl.when(core == 0)
    def _():
        load_cols.wait()
        yi[cz] = wc[...].astype(BF16)

    @pl.when(cy == 0)
    def _():
        load_rows.wait()
        for q in range(S):
            for h in range(2):
                rs[q, h] = wr[q * 32 : (q + 1) * 32, h * 512 : (h + 1) * 512].astype(BF16)
        r0[0, cx] = wr[0:32, 0:512].astype(BF16)
        r1[cx, 0] = wr[0:32, 512:1024].astype(BF16)

    @pl.when(core == 0)
    def _():
        for d in range(1, S):
            cols_out(d, {"col": (cz + d) % S * 2}).start()
        cols_out(0, partner).start()
        start_scatter()

        @pl.when(cy != 0)
        def _():
            block_y(0).wait_recv()

        for d in range(1, 16):
            block_out(d, in_slab(d)[2]).start()
        block_out(0, partner).start()
        start_a()
        for d in range(1, S):
            oz = (cz + d) % S
            cols_in(oz, yi_send.at[0]).wait_recv()
            cols_in(oz, fi_send.at[d]).start()

    @pl.when(core == 1)
    def _():
        start_scatter()
        start_a()
        for oz in range(S):
            cols_in(oz, yi_send.at[0]).wait_recv()
        block_in(cx, cz, p2_send.at[0], partner).wait_recv()

    here = cx * S + cz

    def take(d):
        ox, oz, _ = in_slab(d)
        block_in(ox, oz, p2_send.at[0], partner).wait_recv()

        @pl.when(core == 0)
        def _():
            block_in(ox, oz, pf_send.at[d], partner).start()

    def take_other(d):
        @pl.when((here + d) % 16 != 0)
        def _():
            take(d)

    def rows_of(i):
        return pl.ds(i * B, B)

    def column(s, i):
        return y.at[s // 2, rows_of(i), pl.ds(s % 2 * B, B)]

    def update(s, i, which=(0, 1)):
        left = enc_left(column(s, i)[...])
        for u in which:
            y[u, rows_of(i), :] = min_plus(left, enc_row[s % 2, u], y[u, rows_of(i), :])

    def panel(s, block):
        column(s, s)[...] = block
        closed = enc_left(block)
        for u in range(2):
            old = y[u, rows_of(s), :]
            new = min_plus(closed, jnp.concatenate(enc_right(old), 0), old)
            y[u, rows_of(s), :] = new
            ceil, floor = enc_right(new)
            enc_row[s % 2, u, 0:B, :] = ceil
            enc_row[s % 2, u, B : 2 * B, :] = floor

    @pl.when(here != 0)
    def _():
        take((16 - here) % 16)

    def square_and_take(i, block):
        block = min_plus_block(block)
        for d in range(3):
            take_other(1 + 3 * i + d)
        return block

    block = lax.fori_loop(0, 5, square_and_take, yp[0, 0].astype(F32) - 1.0)
    start_b()
    block = min_plus_block(block)

    for t in range(S):
        lanes = slice(t % 2 * B, (t % 2 + 1) * B)
        for s in range(S):
            y[t // 2, s * B : (s + 1) * B, lanes] = yp[t, s].astype(F32) - 1.0
        y[t // 2, S * B :, lanes] = yi[t].astype(F32) - 1.0

    for s in range(S - 1):
        panel(s, block)
        near = (s + 1) // 2
        update(s, s + 1, (near,))
        block = column(s + 1, s + 1)[...]
        rest = [(s + 1, (1 - near,))] + [(i, (0, 1)) for i in range(s + 2, 2 * S)]
        done = 0
        for q in range(6):
            block = min_plus_block(block)
            until = -(-len(rest) * (q + 1) // 6)
            for i, which in rest[done:until]:
                update(s, i, which)
            done = until
    panel(S - 1, block)
    for i in range(S, 2 * S):
        update(S - 1, i)
    for t in range(S):
        x_ref[t] = y[t // 2, S * B :, t % 2 * B : (t % 2 + 1) * B].astype(BF16)

    for d in range(1, S):
        for copy in stage_b(d, (cx + d) % S, (cy + d) % S):
            copy.wait_recv()

    @pl.when(core == 0)
    def _():
        @pl.when(cy == 0)
        def _():
            for d in range(1, S):
                block_y(d).wait_send()

        for d in range(16):
            block_out(d, partner).wait_send()
        for d in range(S):
            cols_out(d, partner).wait_send()
        for d in range(1, S):
            cols_in((cz + d) % S, fi_send.at[d]).wait_send()
        for d in range(1, 16):
            ox, oz, _ = in_slab(d)
            block_in(ox, oz, pf_send.at[d], partner).wait_send()

    @pl.when(cy == 0)
    def _():
      for q in range(1, S):
          for copy in scatter(q):
              copy.wait_send()

    for d in range(1, S):
      for copy in stage_a(d, cx, cy):
          copy.wait_send()
    for d in range(1, S):
      for copy in stage_b(d, cx, cy):
          copy.wait_send()


def product_kernel(w, x_ref, r0, r1, o_hbm, o, enc_r, o_sem):
    row, col = lax.axis_index("row"), lax.axis_index("col")
    wide = 2 * B
    parts = [pl.ds(j * wide, wide) for j in range(w.shape[1] // wide)]
    stores = [pltpu.make_async_copy(o.at[:, p], o_hbm.at[:, p], o_sem.at[j]) for j, p in enumerate(parts)]

    def encode_strip(s, _):
        for q in range(S):
            for h, part in ((0, r0[q, s]), (1, r1[s, q])):
                ceil, floor = enc_right(part.astype(F32) - 1.0)
                enc_r[s, q * 32 : (q + 1) * 32, h * 512 : (h + 1) * 512] = ceil
                enc_r[s, B + q * 32 : B + (q + 1) * 32, h * 512 : (h + 1) * 512] = floor
        return 0

    lax.fori_loop(0, S, encode_strip, 0)
    lefts = []
    for s in range(S):
        (f0, c0), (f1, c1) = enc_left(x_ref[s].astype(F32))
        lefts.append((f0, f1, c0, c1))
    for j, p in enumerate(parts):
        floors = ceils = None
        for s in range(S):
            right = enc_r[s, :, p]
            f0, f1, c0, c1 = (dot(left, right) for left in lefts[s])
            df, dc = jnp.maximum(f0, f1), jnp.maximum(c0, c1)
            floors = df if floors is None else jnp.maximum(floors, df)
            ceils = dc if ceils is None else jnp.maximum(ceils, dc)
        old = w[:, p]
        new = jnp.minimum(old.astype(F32), decode(floors, ceils, 2.0)).astype(jnp.int32)
        lag = lax.broadcasted_iota(jnp.int32, old.shape, 1) - lax.broadcasted_iota(jnp.int32, old.shape, 0)
        o[:, p] = jnp.where(lag == row * w.shape[0] - col * w.shape[1] - j * wide, 0, new)
        stores[j].start()
    for store in stores:
        store.wait()


def per_device(weights):
    dma = pltpu.SemaphoreType.DMA
    vmem = pl.BlockSpec(memory_space=pltpu.VMEM)
    rows, cols = weights.shape
    closed, r0, r1 = pl.pallas_call(
        gather_kernel,
        out_shape=(
            jax.ShapeDtypeStruct((S, rows, B), BF16),
            jax.ShapeDtypeStruct((S, S, 32, 512), BF16),
            jax.ShapeDtypeStruct((S, S, 32, 512), BF16),
        ),
        in_specs=[pl.BlockSpec(memory_space=pltpu.HBM)],
        out_specs=(vmem, vmem, vmem),
        scratch_shapes=[
            pltpu.VMEM((B, B), jnp.int32),
            pltpu.VMEM((B, cols), jnp.int32),
            pltpu.VMEM((rows, B), jnp.int32),
            pltpu.VMEM((S, 2, 32, 512), BF16),
            pltpu.VMEM((S, S, B, B), BF16),
            pltpu.VMEM((S, rows, B), BF16),
            pltpu.VMEM((2, 1024, 2 * B), F32),
            pltpu.VMEM((2, 2, 2 * B, 2 * B), BF16),
            dma((3,)), dma((S,)), dma, dma((16,)), dma((16,)), dma((16,)), dma((S,)), dma((S,)), dma((S,)),
            dma((S,)), dma, dma((S,)), dma,
            dma((S,)), dma((S,)), dma((S,)), dma((S,)), dma((S,)), dma((S,)), dma((S,)), dma((S,)),
        ],
        compiler_params=pltpu.CompilerParams(
            collective_id=0, has_side_effects=True, vmem_limit_bytes=24 * 2**20
        ),
        name="gather",
    )(pltpu.with_memory_space_constraint(weights, pltpu.HBM))
    return pl.pallas_call(
        product_kernel,
        out_shape=jax.ShapeDtypeStruct(weights.shape, jnp.int32),
        in_specs=[vmem] * 4,
        out_specs=pl.BlockSpec(memory_space=pltpu.HBM),
        scratch_shapes=[
            pltpu.VMEM((rows, cols), jnp.int32),
            pltpu.VMEM((S, 2 * B, cols), BF16),
            dma((4,)),
        ],
        compiler_params=pltpu.CompilerParams(vmem_limit_bytes=32 * 2**20),
        name="product",
    )(weights, closed, r0, r1)


def solution(mesh):
    return jax.shard_map(
        per_device, mesh=mesh, in_specs=(P("row", "col"),), out_specs=P("row", "col"), check_vma=False
    )
```

```python
import math

import jax
import jax.numpy as jnp
from jax import lax
from jax.experimental import pallas as pl
from jax.experimental.pallas import tpu as pltpu
from jax.sharding import PartitionSpec as P

F32 = jnp.float32
BF16 = jnp.bfloat16
MESH = pl.DeviceIdType.MESH
ALPHA = 60.25
BETA = 6.2
SHIFT = 0.984
STEP = 2.0**-BETA
B = 128
S = 4


LOG = 1.0 / (BETA * math.log(2.0))
FLOOR = 2 * ALPHA / BETA + SHIFT


def encode(t):
    u = t * 0.5
    half = jnp.floor(u)
    return jnp.exp2(half * -BETA + ALPHA), u > half


def enc_right(t):
    e, odd = encode(t)
    return jnp.where(odd, e * STEP, e).astype(BF16), e.astype(BF16)


def split_left(t):
    e, odd = encode(t)
    odd_floor = jnp.where(odd, e, 0.0)
    return tuple(u.astype(BF16) for u in (odd_floor, jnp.where(odd, 0.0, e), odd_floor * STEP))


def enc_left(t):
    first = jnp.where(lax.broadcasted_iota(jnp.int32, t.shape, 1) < B // 2, 1.0, 0.0)
    pairs = []
    parts = split_left(t)
    for keep in (first.astype(BF16), (1.0 - first).astype(BF16)):
        of, ev, oc = (u * keep for u in parts)
        pairs.append((jnp.concatenate([of, ev], 1), jnp.concatenate([ev, oc], 1)))
    return pairs


def dot(left, right):
    return jnp.dot(left, right, preferred_element_type=F32)


def decode(floors, ceils, bias):
    low = jnp.floor(FLOOR - jnp.log(floors) * LOG)
    high = jnp.floor(FLOOR + bias - jnp.log(ceils) * LOG)
    return low + jnp.minimum(high, low + (1.0 + bias))


def min_plus(left, right, old):
    (f0, c0), (f1, c1) = left
    floors = jnp.maximum(dot(f0, right), dot(f1, right))
    ceils = jnp.maximum(dot(c0, right), dot(c1, right))
    return jnp.minimum(old, decode(floors, ceils, 1.0))


def min_plus_block(block):
    of, ev, oc = split_left(block)
    ceil, floor = enc_right(block)
    none = jnp.zeros((B // 2, B), BF16)
    first = jnp.concatenate([ceil[: B // 2], none, floor[: B // 2], none], 0)
    second = jnp.concatenate([none, ceil[B // 2 :], none, floor[B // 2 :]], 0)
    right = jnp.concatenate([first, second], 1)
    floors = dot(jnp.concatenate([of, ev], 1), right)
    ceils = dot(jnp.concatenate([ev, oc], 1), right)
    floors = jnp.maximum(floors[:, :B], floors[:, B:])
    ceils = jnp.maximum(ceils[:, :B], ceils[:, B:])
    return jnp.minimum(block, decode(floors, ceils, 1.0))


def remote(src, dst, send, recv, where):
    return pltpu.make_async_remote_copy(
        src_ref=src, dst_ref=dst, send_sem=send, recv_sem=recv, device_id=where, device_id_type=MESH
    )


def gather_kernel(
    w_hbm, x_ref, r0, r1, wp, wr, wc, rs, yp, yi, y, enc_row,
    w_sem, p1_send, p1_recv, p2_send, p2_recv, pf_send, yi_send, yi_recv, fi_send,
    s0_send, s0_recv, s1_send, s1_recv, a0_send, a0_recv, a1_send, a1_recv, b0_send, b0_recv, b1_send, b1_recv,
):
    row, col = lax.axis_index("row"), lax.axis_index("col")
    cx, cy = row // S, row % S
    cz, core = col // 2, col % 2
    block_owner = jnp.logical_and(cy == 0, core == 0)

    def at_x(x):
        return {"row": x * S + cy}

    def at_y(v):
        return {"row": cx * S + v}

    def in_slab(d):
        other = (cx * S + cz + d) % 16
        ox, oz = other // S, other % S
        return ox, oz, {"row": ox * S + cy, "col": oz * 2 + core}

    partner = {"col": cz * 2 + (1 - core)}

    barrier = pltpu.get_barrier_semaphore()

    def greet(where):
        pl.semaphore_signal(barrier, inc=1, device_id=where, device_id_type=MESH)

    for d in range(1, S):
        greet(at_y((cy + d) % S))
    for d in range(1, 16):
        greet(in_slab(d)[2])
    greet(partner)

    load_block = pltpu.make_async_copy(w_hbm.at[pl.ds(0, B), pl.ds(0, B)], wp, w_sem.at[0])
    load_rows = pltpu.make_async_copy(w_hbm.at[pl.ds(0, B)], wr, w_sem.at[1])
    load_cols = pltpu.make_async_copy(w_hbm.at[:, pl.ds(0, B)], wc, w_sem.at[2])

    @pl.when(block_owner)
    def _():
        load_block.start()

    @pl.when(cy == 0)
    def _():
        load_rows.start()

    @pl.when(core == 0)
    def _():
        load_cols.start()

    @pl.when(block_owner)
    def _():
        load_block.wait()
        yp[cz, cx] = wp[...].astype(BF16)

    pl.semaphore_wait(barrier, 19)

    def block_y(d):
        return remote(yp.at[cz, cx], yp.at[cz, cx], p1_send.at[d], p1_recv, at_y((cy + d) % S))

    def block_out(d, where):
        return remote(yp.at[cz, cx], yp.at[cz, cx], p2_send.at[d], p2_recv.at[cz * S + cx], where)

    def block_in(ox, oz, send, where):
        return remote(yp.at[oz, ox], yp.at[oz, ox], send, p2_recv.at[oz * S + ox], where)

    def cols_out(d, where):
        return remote(yi.at[cz], yi.at[cz], yi_send.at[d], yi_recv.at[cz], where)

    def cols_in(oz, send):
        return remote(yi.at[oz], yi.at[oz], send, yi_recv.at[oz], partner)

    def scatter(q):
        return (
            remote(rs.at[q, 0], r0.at[q, cx], s0_send.at[q], s0_recv, at_y(q)),
            remote(rs.at[q, 1], r1.at[cx, q], s1_send.at[q], s1_recv, at_y(q)),
        )

    def stage_a(d, x, v):
        return (
            remote(r0.at[cy, x], r0.at[cy, x], a0_send.at[d], a0_recv.at[x], at_x((cx + d) % S)),
            remote(r1.at[cx, v], r1.at[cx, v], a1_send.at[d], a1_recv.at[v], at_y((cy + d) % S)),
        )

    def stage_b(d, x, v):
        return (
            remote(r0.at[v], r0.at[v], b0_send.at[d], b0_recv.at[v], at_y((cy + d) % S)),
            remote(r1.at[x], r1.at[x], b1_send.at[d], b1_recv.at[x], at_x((cx + d) % S)),
        )

    def start_scatter():
        @pl.when(cy == 0)
        def _():
            for q in range(1, S):
                for copy in scatter(q):
                    copy.start()

    def start_a():
        @pl.when(cy != 0)
        def _():
            for copy in scatter(cy):
                copy.wait_recv()

        for d in range(1, S):
            for copy in stage_a(d, cx, cy):
                copy.start()

    def start_b(half):
        for d in range(1, S):
            stage_a(d, (cx + d) % S, (cy + d) % S)[half].wait_recv()
        for d in range(1, S):
            stage_b(d, cx, cy)[half].start()

    @pl.when(block_owner)
    def _():
        for d in range(1, S):
            block_y(d).start()

    @pl.when(core == 0)
    def _():
        load_cols.wait()
        yi[cz] = wc[...].astype(BF16)

    @pl.when(cy == 0)
    def _():
        load_rows.wait()
        for q in range(S):
            for h in range(2):
                rs[q, h] = wr[q * 32 : (q + 1) * 32, h * 512 : (h + 1) * 512].astype(BF16)
        r0[0, cx] = wr[0:32, 0:512].astype(BF16)
        r1[cx, 0] = wr[0:32, 512:1024].astype(BF16)

    @pl.when(core == 0)
    def _():
        for d in range(1, S):
            cols_out(d, {"col": (cz + d) % S * 2}).start()
        cols_out(0, partner).start()
        start_scatter()

        @pl.when(cy != 0)
        def _():
            block_y(0).wait_recv()

        for d in range(1, 16):
            block_out(d, in_slab(d)[2]).start()
        block_out(0, partner).start()
        start_a()
        for d in range(1, S):
            oz = (cz + d) % S
            cols_in(oz, yi_send.at[0]).wait_recv()
            cols_in(oz, fi_send.at[d]).start()

    @pl.when(core == 1)
    def _():
        start_scatter()
        start_a()
        for oz in range(S):
            cols_in(oz, yi_send.at[0]).wait_recv()
        block_in(cx, cz, p2_send.at[0], partner).wait_recv()

    here = cx * S + cz

    def take(d):
        ox, oz, _ = in_slab(d)
        block_in(ox, oz, p2_send.at[0], partner).wait_recv()

        @pl.when(core == 0)
        def _():
            block_in(ox, oz, pf_send.at[d], partner).start()

    def take_other(d):
        @pl.when((here + d) % 16 != 0)
        def _():
            take(d)

    def rows_of(i):
        return pl.ds(i * B, B)

    def column(s, i):
        return y.at[s // 2, rows_of(i), pl.ds(s % 2 * B, B)]

    def update(s, i, which=(0, 1)):
        left = enc_left(column(s, i)[...])
        for u in which:
            y[u, rows_of(i), :] = min_plus(left, enc_row[s % 2, u], y[u, rows_of(i), :])

    def panel(s, block):
        column(s, s)[...] = block
        closed = enc_left(block)
        for u in range(2):
            old = y[u, rows_of(s), :]
            new = min_plus(closed, jnp.concatenate(enc_right(old), 0), old)
            y[u, rows_of(s), :] = new
            ceil, floor = enc_right(new)
            enc_row[s % 2, u, 0:B, :] = ceil
            enc_row[s % 2, u, B : 2 * B, :] = floor

    start_b(0)

    @pl.when(here != 0)
    def _():
        take((16 - here) % 16)

    def square_and_take(i, block):
        block = min_plus_block(block)
        for d in range(3):
            take_other(1 + 3 * i + d)
        return block

    block = lax.fori_loop(0, 5, square_and_take, yp[0, 0].astype(F32) - 1.0)
    start_b(1)
    block = min_plus_block(block)

    for t in range(S):
        lanes = slice(t % 2 * B, (t % 2 + 1) * B)
        for s in range(S):
            y[t // 2, s * B : (s + 1) * B, lanes] = yp[t, s].astype(F32) - 1.0
        y[t // 2, S * B :, lanes] = yi[t].astype(F32) - 1.0

    for s in range(S - 1):
        panel(s, block)
        near = (s + 1) // 2
        update(s, s + 1, (near,))
        block = column(s + 1, s + 1)[...]
        rest = [(s + 1, (1 - near,))] + [(i, (0, 1)) for i in range(s + 2, 2 * S)]
        done = 0
        for q in range(6):
            block = min_plus_block(block)
            until = -(-len(rest) * (q + 1) // 6)
            for i, which in rest[done:until]:
                update(s, i, which)
            done = until
    panel(S - 1, block)
    for i in range(S, 2 * S):
        update(S - 1, i)
    for t in range(S):
        x_ref[t] = y[t // 2, S * B :, t % 2 * B : (t % 2 + 1) * B].astype(BF16)

    for d in range(1, S):
        for copy in stage_b(d, (cx + d) % S, (cy + d) % S):
            copy.wait_recv()

    @pl.when(core == 0)
    def _():
        @pl.when(cy == 0)
        def _():
            for d in range(1, S):
                block_y(d).wait_send()

        for d in range(16):
            block_out(d, partner).wait_send()
        for d in range(S):
            cols_out(d, partner).wait_send()
        for d in range(1, S):
            cols_in((cz + d) % S, fi_send.at[d]).wait_send()
        for d in range(1, 16):
            ox, oz, _ = in_slab(d)
            block_in(ox, oz, pf_send.at[d], partner).wait_send()

    @pl.when(cy == 0)
    def _():
      for q in range(1, S):
          for copy in scatter(q):
              copy.wait_send()

    for d in range(1, S):
      for copy in stage_a(d, cx, cy):
          copy.wait_send()
    for d in range(1, S):
      for copy in stage_b(d, cx, cy):
          copy.wait_send()


def product_kernel(w, x_ref, r0, r1, o_hbm, o, o_sem):
    row, col = lax.axis_index("row"), lax.axis_index("col")
    wide = 2 * B
    parts = [pl.ds(j * wide, wide) for j in range(w.shape[1] // wide)]
    stores = [pltpu.make_async_copy(o.at[:, p], o_hbm.at[:, p], o_sem.at[j]) for j, p in enumerate(parts)]

    def right_operand(s, j):
        lanes = pl.ds(j % 2 * wide, wide)
        quarters = [(r0[q, s, :, lanes] if j < 2 else r1[s, q, :, lanes]) for q in range(S)]
        return jnp.concatenate(enc_right(jnp.concatenate(quarters, 0).astype(F32) - 1.0), 0)

    lefts = []
    for s in range(S):
        (f0, c0), (f1, c1) = enc_left(x_ref[s].astype(F32))
        lefts.append((f0, f1, c0, c1))
    for j, p in enumerate(parts):
        floors = ceils = None
        for s in range(S):
            right = right_operand(s, j)
            f0, f1, c0, c1 = (dot(left, right) for left in lefts[s])
            df, dc = jnp.maximum(f0, f1), jnp.maximum(c0, c1)
            floors = df if floors is None else jnp.maximum(floors, df)
            ceils = dc if ceils is None else jnp.maximum(ceils, dc)
        old = w[:, p]
        new = jnp.minimum(old.astype(F32), decode(floors, ceils, 2.0)).astype(jnp.int32)
        lag = lax.broadcasted_iota(jnp.int32, old.shape, 1) - lax.broadcasted_iota(jnp.int32, old.shape, 0)
        o[:, p] = jnp.where(lag == row * w.shape[0] - col * w.shape[1] - j * wide, 0, new)
        stores[j].start()
    for store in stores:
        store.wait()


def per_device(weights):
    dma = pltpu.SemaphoreType.DMA
    vmem = pl.BlockSpec(memory_space=pltpu.VMEM)
    rows, cols = weights.shape
    closed, r0, r1 = pl.pallas_call(
        gather_kernel,
        out_shape=(
            jax.ShapeDtypeStruct((S, rows, B), BF16),
            jax.ShapeDtypeStruct((S, S, 32, 512), BF16),
            jax.ShapeDtypeStruct((S, S, 32, 512), BF16),
        ),
        in_specs=[pl.BlockSpec(memory_space=pltpu.HBM)],
        out_specs=(vmem, vmem, vmem),
        scratch_shapes=[
            pltpu.VMEM((B, B), jnp.int32),
            pltpu.VMEM((B, cols), jnp.int32),
            pltpu.VMEM((rows, B), jnp.int32),
            pltpu.VMEM((S, 2, 32, 512), BF16),
            pltpu.VMEM((S, S, B, B), BF16),
            pltpu.VMEM((S, rows, B), BF16),
            pltpu.VMEM((2, 1024, 2 * B), F32),
            pltpu.VMEM((2, 2, 2 * B, 2 * B), BF16),
            dma((3,)), dma((S,)), dma, dma((16,)), dma((16,)), dma((16,)), dma((S,)), dma((S,)), dma((S,)),
            dma((S,)), dma, dma((S,)), dma,
            dma((S,)), dma((S,)), dma((S,)), dma((S,)), dma((S,)), dma((S,)), dma((S,)), dma((S,)),
        ],
        compiler_params=pltpu.CompilerParams(
            collective_id=0, has_side_effects=True, vmem_limit_bytes=24 * 2**20
        ),
        name="gather",
    )(pltpu.with_memory_space_constraint(weights, pltpu.HBM))
    return pl.pallas_call(
        product_kernel,
        out_shape=jax.ShapeDtypeStruct(weights.shape, jnp.int32),
        in_specs=[vmem] * 4,
        out_specs=pl.BlockSpec(memory_space=pltpu.HBM),
        scratch_shapes=[
            pltpu.VMEM((rows, cols), jnp.int32),
            dma((4,)),
        ],
        compiler_params=pltpu.CompilerParams(vmem_limit_bytes=32 * 2**20),
        name="product",
    )(weights, closed, r0, r1)


def solution(mesh):
    return jax.shard_map(
        per_device, mesh=mesh, in_specs=(P("row", "col"),), out_specs=P("row", "col"), check_vma=False
    )
```

```python
import math

import jax
import jax.numpy as jnp
from jax import lax
from jax.experimental import pallas as pl
from jax.experimental.pallas import tpu as pltpu
from jax.sharding import PartitionSpec as P

F32 = jnp.float32
BF16 = jnp.bfloat16
MESH = pl.DeviceIdType.MESH
ALPHA = 60.25
BETA = 6.2
SHIFT = 0.984
STEP = 2.0**-BETA
B = 128
S = 4


LOG = 1.0 / (BETA * math.log(2.0))
FLOOR = 2 * ALPHA / BETA + SHIFT


def encode(t):
    u = t * 0.5
    half = jnp.floor(u)
    return jnp.exp2(half * -BETA + ALPHA), u > half


def enc_right(t):
    e, odd = encode(t)
    return jnp.where(odd, e * STEP, e).astype(BF16), e.astype(BF16)


def split_left(t):
    e, odd = encode(t)
    odd_floor = jnp.where(odd, e, 0.0)
    return tuple(u.astype(BF16) for u in (odd_floor, jnp.where(odd, 0.0, e), odd_floor * STEP))


def enc_left(t):
    first = jnp.where(lax.broadcasted_iota(jnp.int32, t.shape, 1) < B // 2, 1.0, 0.0)
    pairs = []
    parts = split_left(t)
    for keep in (first.astype(BF16), (1.0 - first).astype(BF16)):
        of, ev, oc = (u * keep for u in parts)
        pairs.append((jnp.concatenate([of, ev], 1), jnp.concatenate([ev, oc], 1)))
    return pairs


def dot(left, right):
    return jnp.dot(left, right, preferred_element_type=F32)


def decode(floors, ceils, bias):
    low = jnp.floor(FLOOR - jnp.log(floors) * LOG)
    high = jnp.floor(FLOOR + bias - jnp.log(ceils) * LOG)
    return low + jnp.minimum(high, low + (1.0 + bias))


def min_plus(left, right, old):
    (f0, c0), (f1, c1) = left
    floors = jnp.maximum(dot(f0, right), dot(f1, right))
    ceils = jnp.maximum(dot(c0, right), dot(c1, right))
    return jnp.minimum(old, decode(floors, ceils, 1.0))


def min_plus_block(block):
    of, ev, oc = split_left(block)
    ceil, floor = enc_right(block)
    none = jnp.zeros((B // 2, B), BF16)
    first = jnp.concatenate([ceil[: B // 2], none, floor[: B // 2], none], 0)
    second = jnp.concatenate([none, ceil[B // 2 :], none, floor[B // 2 :]], 0)
    right = jnp.concatenate([first, second], 1)
    floors = dot(jnp.concatenate([of, ev], 1), right)
    ceils = dot(jnp.concatenate([ev, oc], 1), right)
    floors = jnp.maximum(floors[:, :B], floors[:, B:])
    ceils = jnp.maximum(ceils[:, :B], ceils[:, B:])
    return jnp.minimum(block, decode(floors, ceils, 1.0))


def remote(src, dst, send, recv, where):
    return pltpu.make_async_remote_copy(
        src_ref=src, dst_ref=dst, send_sem=send, recv_sem=recv, device_id=where, device_id_type=MESH
    )


def gather_kernel(
    w_hbm, x_ref, r0, r1, wp, wr, wc, rs, yp, yi, y, enc_row,
    w_sem, p1_send, p1_recv, p2_send, p2_recv, pf_send, yi_send, yi_recv, fi_send,
    s0_send, s0_recv, s1_send, s1_recv, a0_send, a0_recv, a1_send, a1_recv, b0_send, b0_recv, b1_send, b1_recv,
):
    row, col = lax.axis_index("row"), lax.axis_index("col")
    cx, cy = row // S, row % S
    cz, core = col // 2, col % 2
    block_owner = jnp.logical_and(cy == 0, core == 0)

    def at_x(x):
        return {"row": x * S + cy}

    def at_y(v):
        return {"row": cx * S + v}

    def in_slab(d):
        other = (cx * S + cz + d) % 16
        ox, oz = other // S, other % S
        return ox, oz, {"row": ox * S + cy, "col": oz * 2 + core}

    partner = {"col": cz * 2 + (1 - core)}

    barrier = pltpu.get_barrier_semaphore()

    def greet(where):
        pl.semaphore_signal(barrier, inc=1, device_id=where, device_id_type=MESH)

    for d in range(1, S):
        greet(at_y((cy + d) % S))
    for d in range(1, 16):
        greet(in_slab(d)[2])
    greet(partner)

    load_block = pltpu.make_async_copy(w_hbm.at[pl.ds(0, B), pl.ds(0, B)], wp, w_sem.at[0])
    load_rows = pltpu.make_async_copy(w_hbm.at[pl.ds(0, B)], wr, w_sem.at[1])
    load_cols = pltpu.make_async_copy(w_hbm.at[:, pl.ds(0, B)], wc, w_sem.at[2])

    @pl.when(block_owner)
    def _():
        load_block.start()

    @pl.when(cy == 0)
    def _():
        load_rows.start()

    @pl.when(core == 0)
    def _():
        load_cols.start()

    @pl.when(block_owner)
    def _():
        load_block.wait()
        yp[cz, cx] = wp[...].astype(BF16)

    pl.semaphore_wait(barrier, 19)

    def block_y(d):
        return remote(yp.at[cz, cx], yp.at[cz, cx], p1_send.at[d], p1_recv, at_y((cy + d) % S))

    def block_out(d, where):
        return remote(yp.at[cz, cx], yp.at[cz, cx], p2_send.at[d], p2_recv.at[cz * S + cx], where)

    def block_in(ox, oz, send, where):
        return remote(yp.at[oz, ox], yp.at[oz, ox], send, p2_recv.at[oz * S + ox], where)

    def cols_out(d, where):
        return remote(yi.at[cz], yi.at[cz], yi_send.at[d], yi_recv.at[cz], where)

    def cols_in(oz, send):
        return remote(yi.at[oz], yi.at[oz], send, yi_recv.at[oz], partner)

    def scatter(q):
        return (
            remote(rs.at[q, 0], r0.at[q, cx], s0_send.at[q], s0_recv, at_y(q)),
            remote(rs.at[q, 1], r1.at[cx, q], s1_send.at[q], s1_recv, at_y(q)),
        )

    def stage_a(d, x, v):
        return (
            remote(r0.at[cy, x], r0.at[cy, x], a0_send.at[d], a0_recv.at[x], at_x((cx + d) % S)),
            remote(r1.at[cx, v], r1.at[cx, v], a1_send.at[d], a1_recv.at[v], at_y((cy + d) % S)),
        )

    def stage_b(d, x, v):
        return (
            remote(r0.at[v], r0.at[v], b0_send.at[d], b0_recv.at[v], at_y((cy + d) % S)),
            remote(r1.at[x], r1.at[x], b1_send.at[d], b1_recv.at[x], at_x((cx + d) % S)),
        )

    def start_scatter():
        @pl.when(cy == 0)
        def _():
            for q in range(1, S):
                for copy in scatter(q):
                    copy.start()

    def start_a():
        @pl.when(cy != 0)
        def _():
            for copy in scatter(cy):
                copy.wait_recv()

        for d in range(1, S):
            for copy in stage_a(d, cx, cy):
                copy.start()

    def start_b(half):
        for d in range(1, S):
            stage_a(d, (cx + d) % S, (cy + d) % S)[half].wait_recv()
        for d in range(1, S):
            stage_b(d, cx, cy)[half].start()

    @pl.when(block_owner)
    def _():
        for d in range(1, S):
            block_y(d).start()

    @pl.when(core == 0)
    def _():
        load_cols.wait()
        yi[cz] = wc[...].astype(BF16)

    @pl.when(cy == 0)
    def _():
        load_rows.wait()
        for q in range(S):
            for h in range(2):
                rs[q, h] = wr[q * 32 : (q + 1) * 32, h * 512 : (h + 1) * 512].astype(BF16)
        r0[0, cx] = wr[0:32, 0:512].astype(BF16)
        r1[cx, 0] = wr[0:32, 512:1024].astype(BF16)

    @pl.when(core == 0)
    def _():
        for d in range(1, S):
            cols_out(d, {"col": (cz + d) % S * 2}).start()
        cols_out(0, partner).start()
        start_scatter()

        @pl.when(cy != 0)
        def _():
            block_y(0).wait_recv()

        for d in range(1, 16):
            block_out(d, in_slab(d)[2]).start()
        block_out(0, partner).start()
        start_a()
        for d in range(1, S):
            oz = (cz + d) % S
            cols_in(oz, yi_send.at[0]).wait_recv()
            cols_in(oz, fi_send.at[d]).start()

    @pl.when(core == 1)
    def _():
        start_scatter()
        start_a()
        for oz in range(S):
            cols_in(oz, yi_send.at[0]).wait_recv()
        block_in(cx, cz, p2_send.at[0], partner).wait_recv()

    here = cx * S + cz

    def take(d):
        ox, oz, _ = in_slab(d)
        block_in(ox, oz, p2_send.at[0], partner).wait_recv()

        @pl.when(core == 0)
        def _():
            block_in(ox, oz, pf_send.at[d], partner).start()

    def take_other(d):
        @pl.when((here + d) % 16 != 0)
        def _():
            take(d)

    def rows_of(i, count=1):
        return pl.ds(i * B, count * B)

    def column(s, i, count=1):
        return y.at[s // 2, rows_of(i, count), pl.ds(s % 2 * B, B)]

    def update(s, i, which=(0, 1), count=1):
        left = enc_left(column(s, i, count)[...])
        for u in which:
            y[u, rows_of(i, count), :] = min_plus(left, enc_row[s % 2, u], y[u, rows_of(i, count), :])

    def panel(s, block):
        column(s, s)[...] = block
        closed = enc_left(block)
        for u in range(2):
            old = y[u, rows_of(s), :]
            new = min_plus(closed, jnp.concatenate(enc_right(old), 0), old)
            y[u, rows_of(s), :] = new
            ceil, floor = enc_right(new)
            enc_row[s % 2, u, 0:B, :] = ceil
            enc_row[s % 2, u, B : 2 * B, :] = floor

    start_b(0)

    @pl.when(here != 0)
    def _():
        take((16 - here) % 16)

    @pl.when(core == 0)
    def _():
        for d in range(1, 16):
            take_other(d)

    def square_and_take(i, block):
        block = min_plus_block(block)

        @pl.when(core == 1)
        def _():
            for d in range(3):
                take_other(1 + 3 * i + d)

        return block

    block = lax.fori_loop(0, 5, square_and_take, yp[0, 0].astype(F32) - 1.0)
    start_b(1)
    block = min_plus_block(block)

    for t in range(S):
        lanes = slice(t % 2 * B, (t % 2 + 1) * B)
        for s in range(S):
            y[t // 2, s * B : (s + 1) * B, lanes] = yp[t, s].astype(F32) - 1.0
        y[t // 2, S * B :, lanes] = yi[t].astype(F32) - 1.0

    for s in range(S - 1):
        panel(s, block)
        near = (s + 1) // 2
        update(s, s + 1, (near,))
        block = column(s + 1, s + 1)[...]
        rest = [(s + 1, (1 - near,))] + [(i, (0, 1)) for i in range(s + 2, 2 * S)]
        done = 0
        for q in range(6):
            block = min_plus_block(block)
            until = -(-len(rest) * (q + 1) // 6)
            for i, which in rest[done:until]:
                update(s, i, which)
            done = until
    panel(S - 1, block)
    for i in range(S, 2 * S, 4):
        update(S - 1, i, count=4)
    for t in range(S):
        x_ref[t] = y[t // 2, S * B :, t % 2 * B : (t % 2 + 1) * B].astype(BF16)

    for d in range(1, S):
        for copy in stage_b(d, (cx + d) % S, (cy + d) % S):
            copy.wait_recv()

    @pl.when(core == 0)
    def _():
        @pl.when(cy == 0)
        def _():
            for d in range(1, S):
                block_y(d).wait_send()

        for d in range(16):
            block_out(d, partner).wait_send()
        for d in range(S):
            cols_out(d, partner).wait_send()
        for d in range(1, S):
            cols_in((cz + d) % S, fi_send.at[d]).wait_send()
        for d in range(1, 16):
            ox, oz, _ = in_slab(d)
            block_in(ox, oz, pf_send.at[d], partner).wait_send()

    @pl.when(cy == 0)
    def _():
      for q in range(1, S):
          for copy in scatter(q):
              copy.wait_send()

    for d in range(1, S):
      for copy in stage_a(d, cx, cy):
          copy.wait_send()
    for d in range(1, S):
      for copy in stage_b(d, cx, cy):
          copy.wait_send()


def product_kernel(w, x_ref, r0, r1, o_hbm, o, o_sem):
    row, col = lax.axis_index("row"), lax.axis_index("col")
    wide = 2 * B
    parts = [pl.ds(j * wide, wide) for j in range(w.shape[1] // wide)]
    stores = [pltpu.make_async_copy(o.at[:, p], o_hbm.at[:, p], o_sem.at[j]) for j, p in enumerate(parts)]

    def right_operand(s, j):
        lanes = pl.ds(j % 2 * wide, wide)
        quarters = [(r0[q, s, :, lanes] if j < 2 else r1[s, q, :, lanes]) for q in range(S)]
        return jnp.concatenate(enc_right(jnp.concatenate(quarters, 0).astype(F32) - 1.0), 0)

    lefts = []
    for s in range(S):
        (f0, c0), (f1, c1) = enc_left(x_ref[s].astype(F32))
        lefts.append((f0, f1, c0, c1))
    for j, p in enumerate(parts):
        floors = ceils = None
        for s in range(S):
            right = right_operand(s, j)
            f0, f1, c0, c1 = (dot(left, right) for left in lefts[s])
            df, dc = jnp.maximum(f0, f1), jnp.maximum(c0, c1)
            floors = df if floors is None else jnp.maximum(floors, df)
            ceils = dc if ceils is None else jnp.maximum(ceils, dc)
        old = w[:, p]
        new = jnp.minimum(old.astype(F32), decode(floors, ceils, 2.0)).astype(jnp.int32)
        lag = lax.broadcasted_iota(jnp.int32, old.shape, 1) - lax.broadcasted_iota(jnp.int32, old.shape, 0)
        o[:, p] = jnp.where(lag == row * w.shape[0] - col * w.shape[1] - j * wide, 0, new)
        stores[j].start()
    for store in stores:
        store.wait()


def per_device(weights):
    dma = pltpu.SemaphoreType.DMA
    vmem = pl.BlockSpec(memory_space=pltpu.VMEM)
    rows, cols = weights.shape
    closed, r0, r1 = pl.pallas_call(
        gather_kernel,
        out_shape=(
            jax.ShapeDtypeStruct((S, rows, B), BF16),
            jax.ShapeDtypeStruct((S, S, 32, 512), BF16),
            jax.ShapeDtypeStruct((S, S, 32, 512), BF16),
        ),
        in_specs=[pl.BlockSpec(memory_space=pltpu.HBM)],
        out_specs=(vmem, vmem, vmem),
        scratch_shapes=[
            pltpu.VMEM((B, B), jnp.int32),
            pltpu.VMEM((B, cols), jnp.int32),
            pltpu.VMEM((rows, B), jnp.int32),
            pltpu.VMEM((S, 2, 32, 512), BF16),
            pltpu.VMEM((S, S, B, B), BF16),
            pltpu.VMEM((S, rows, B), BF16),
            pltpu.VMEM((2, 1024, 2 * B), F32),
            pltpu.VMEM((2, 2, 2 * B, 2 * B), BF16),
            dma((3,)), dma((S,)), dma, dma((16,)), dma((16,)), dma((16,)), dma((S,)), dma((S,)), dma((S,)),
            dma((S,)), dma, dma((S,)), dma,
            dma((S,)), dma((S,)), dma((S,)), dma((S,)), dma((S,)), dma((S,)), dma((S,)), dma((S,)),
        ],
        compiler_params=pltpu.CompilerParams(
            collective_id=0, has_side_effects=True, vmem_limit_bytes=24 * 2**20
        ),
        name="gather",
    )(pltpu.with_memory_space_constraint(weights, pltpu.HBM))
    return pl.pallas_call(
        product_kernel,
        out_shape=jax.ShapeDtypeStruct(weights.shape, jnp.int32),
        in_specs=[vmem] * 4,
        out_specs=pl.BlockSpec(memory_space=pltpu.HBM),
        scratch_shapes=[
            pltpu.VMEM((rows, cols), jnp.int32),
            dma((4,)),
        ],
        compiler_params=pltpu.CompilerParams(vmem_limit_bytes=32 * 2**20),
        name="product",
    )(weights, closed, r0, r1)


def solution(mesh):
    return jax.shard_map(
        per_device, mesh=mesh, in_specs=(P("row", "col"),), out_specs=P("row", "col"), check_vma=False
    )
```

```python
import math

import jax
import jax.numpy as jnp
from jax import lax
from jax.experimental import pallas as pl
from jax.experimental.pallas import tpu as pltpu
from jax.sharding import PartitionSpec as P

F32 = jnp.float32
BF16 = jnp.bfloat16
MESH = pl.DeviceIdType.MESH
ALPHA = 60.25
BETA = 6.2
SHIFT = 0.984
STEP = 2.0**-BETA
B = 128
S = 4


LOG = 1.0 / (BETA * math.log(2.0))
FLOOR = 2 * ALPHA / BETA + SHIFT


def encode(t):
    u = t * 0.5
    half = jnp.floor(u)
    return jnp.exp2(half * -BETA + ALPHA), u > half


def enc_right(t):
    e, odd = encode(t)
    return jnp.where(odd, e * STEP, e).astype(BF16), e.astype(BF16)


def split_left(t):
    e, odd = encode(t)
    odd_floor = jnp.where(odd, e, 0.0)
    return tuple(u.astype(BF16) for u in (odd_floor, jnp.where(odd, 0.0, e), odd_floor * STEP))


def enc_left(t):
    first = jnp.where(lax.broadcasted_iota(jnp.int32, t.shape, 1) < B // 2, 1.0, 0.0)
    pairs = []
    parts = split_left(t)
    for keep in (first.astype(BF16), (1.0 - first).astype(BF16)):
        of, ev, oc = (u * keep for u in parts)
        pairs.append((jnp.concatenate([of, ev], 1), jnp.concatenate([ev, oc], 1)))
    return pairs


def dot(left, right):
    return jnp.dot(left, right, preferred_element_type=F32)


def decode(floors, ceils, bias):
    low = jnp.floor(FLOOR - jnp.log(floors) * LOG)
    high = jnp.floor(FLOOR + bias - jnp.log(ceils) * LOG)
    return low + jnp.minimum(high, low + (1.0 + bias))


def min_plus(left, right, old):
    (f0, c0), (f1, c1) = left
    floors = jnp.maximum(dot(f0, right), dot(f1, right))
    ceils = jnp.maximum(dot(c0, right), dot(c1, right))
    return jnp.minimum(old, decode(floors, ceils, 1.0))


def min_plus_block(block):
    of, ev, oc = split_left(block)
    ceil, floor = enc_right(block)
    none = jnp.zeros((B // 2, B), BF16)
    first = jnp.concatenate([ceil[: B // 2], none, floor[: B // 2], none], 0)
    second = jnp.concatenate([none, ceil[B // 2 :], none, floor[B // 2 :]], 0)
    right = jnp.concatenate([first, second], 1)
    floors = dot(jnp.concatenate([of, ev], 1), right)
    ceils = dot(jnp.concatenate([ev, oc], 1), right)
    floors = jnp.maximum(floors[:, :B], floors[:, B:])
    ceils = jnp.maximum(ceils[:, :B], ceils[:, B:])
    return jnp.minimum(block, decode(floors, ceils, 1.0))


def remote(src, dst, send, recv, where):
    return pltpu.make_async_remote_copy(
        src_ref=src, dst_ref=dst, send_sem=send, recv_sem=recv, device_id=where, device_id_type=MESH
    )


def gather_kernel(
    w_hbm, x_ref, r0, r1, wp, wr, wc, rs, yp, yi, y, enc_row,
    w_sem, p1_send, p1_recv, p2_send, p2_recv, pf_send, yi_send, yi_recv, fi_send,
    s0_send, s0_recv, s1_send, s1_recv, a0_send, a0_recv, a1_send, a1_recv, b0_send, b0_recv, b1_send, b1_recv,
):
    row, col = lax.axis_index("row"), lax.axis_index("col")
    cx, cy = row // S, row % S
    cz, core = col // 2, col % 2
    block_owner = jnp.logical_and(cy == 0, core == 0)

    def at_x(x):
        return {"row": x * S + cy}

    def at_y(v):
        return {"row": cx * S + v}

    def in_slab(d):
        other = (cx * S + cz + d) % 16
        ox, oz = other // S, other % S
        return ox, oz, {"row": ox * S + cy, "col": oz * 2 + core}

    partner = {"col": cz * 2 + (1 - core)}

    barrier = pltpu.get_barrier_semaphore()

    def greet(where):
        pl.semaphore_signal(barrier, inc=1, device_id=where, device_id_type=MESH)

    for d in range(1, S):
        greet(at_y((cy + d) % S))
    for d in range(1, 16):
        greet(in_slab(d)[2])
    greet(partner)

    load_block = pltpu.make_async_copy(w_hbm.at[pl.ds(0, B), pl.ds(0, B)], wp, w_sem.at[0])
    load_rows = pltpu.make_async_copy(w_hbm.at[pl.ds(0, B)], wr, w_sem.at[1])
    load_cols = pltpu.make_async_copy(w_hbm.at[:, pl.ds(0, B)], wc, w_sem.at[2])

    @pl.when(block_owner)
    def _():
        load_block.start()

    @pl.when(cy == 0)
    def _():
        load_rows.start()

    @pl.when(core == 0)
    def _():
        load_cols.start()

    @pl.when(block_owner)
    def _():
        load_block.wait()
        yp[cz, cx] = wp[...].astype(BF16)

    pl.semaphore_wait(barrier, 19)

    def block_y(d):
        return remote(yp.at[cz, cx], yp.at[cz, cx], p1_send.at[d], p1_recv, at_y((cy + d) % S))

    def block_out(d, where):
        return remote(yp.at[cz, cx], yp.at[cz, cx], p2_send.at[d], p2_recv.at[cz * S + cx], where)

    def block_in(ox, oz, send, where):
        return remote(yp.at[oz, ox], yp.at[oz, ox], send, p2_recv.at[oz * S + ox], where)

    def cols_out(d, where):
        return remote(yi.at[cz], yi.at[cz], yi_send.at[d], yi_recv.at[cz], where)

    def cols_in(oz, send):
        return remote(yi.at[oz], yi.at[oz], send, yi_recv.at[oz], partner)

    def scatter(q):
        return (
            remote(rs.at[q, 0], r0.at[q, cx], s0_send.at[q], s0_recv, at_y(q)),
            remote(rs.at[q, 1], r1.at[cx, q], s1_send.at[q], s1_recv, at_y(q)),
        )

    def stage_a(d, x, v):
        return (
            remote(r0.at[cy, x], r0.at[cy, x], a0_send.at[d], a0_recv.at[x], at_x((cx + d) % S)),
            remote(r1.at[cx, v], r1.at[cx, v], a1_send.at[d], a1_recv.at[v], at_y((cy + d) % S)),
        )

    def stage_b(d, x, v):
        return (
            remote(r0.at[v], r0.at[v], b0_send.at[d], b0_recv.at[v], at_y((cy + d) % S)),
            remote(r1.at[x], r1.at[x], b1_send.at[d], b1_recv.at[x], at_x((cx + d) % S)),
        )

    def start_scatter():
        @pl.when(cy == 0)
        def _():
            for q in range(1, S):
                for copy in scatter(q):
                    copy.start()

    def start_a():
        @pl.when(cy != 0)
        def _():
            for copy in scatter(cy):
                copy.wait_recv()

        for d in range(1, S):
            for copy in stage_a(d, cx, cy):
                copy.start()

    def start_b(half):
        for d in range(1, S):
            stage_a(d, (cx + d) % S, (cy + d) % S)[half].wait_recv()
        for d in range(1, S):
            stage_b(d, cx, cy)[half].start()

    @pl.when(block_owner)
    def _():
        for d in range(1, S):
            block_y(d).start()

    @pl.when(core == 0)
    def _():
        load_cols.wait()
        yi[cz] = wc[...].astype(BF16)

    @pl.when(cy == 0)
    def _():
        load_rows.wait()
        for q in range(S):
            for h in range(2):
                rs[q, h] = wr[q * 32 : (q + 1) * 32, h * 512 : (h + 1) * 512].astype(BF16)
        r0[0, cx] = wr[0:32, 0:512].astype(BF16)
        r1[cx, 0] = wr[0:32, 512:1024].astype(BF16)

    @pl.when(core == 0)
    def _():
        for d in range(1, S):
            cols_out(d, {"col": (cz + d) % S * 2}).start()
        cols_out(0, partner).start()
        start_scatter()

        @pl.when(cy != 0)
        def _():
            block_y(0).wait_recv()

        for d in range(1, 16):
            block_out(d, in_slab(d)[2]).start()
        block_out(0, partner).start()
        start_a()
        for d in range(1, S):
            oz = (cz + d) % S
            cols_in(oz, yi_send.at[0]).wait_recv()
            cols_in(oz, fi_send.at[d]).start()

    @pl.when(core == 1)
    def _():
        start_scatter()
        start_a()
        for oz in range(S):
            cols_in(oz, yi_send.at[0]).wait_recv()
        block_in(cx, cz, p2_send.at[0], partner).wait_recv()

    here = cx * S + cz

    def take(d):
        ox, oz, _ = in_slab(d)
        block_in(ox, oz, p2_send.at[0], partner).wait_recv()

        @pl.when(core == 0)
        def _():
            block_in(ox, oz, pf_send.at[d], partner).start()

    def take_other(d):
        @pl.when((here + d) % 16 != 0)
        def _():
            take(d)

    def rows_of(i, count=1):
        return pl.ds(i * B, count * B)

    def column(s, i, count=1):
        return y.at[s // 2, rows_of(i, count), pl.ds(s % 2 * B, B)]

    def update(s, i, which=(0, 1), count=1):
        left = enc_left(column(s, i, count)[...])
        for u in which:
            y[u, rows_of(i, count), :] = min_plus(left, enc_row[s % 2, u], y[u, rows_of(i, count), :])

    def panel(s, block):
        column(s, s)[...] = block
        closed = enc_left(block)
        for u in range(2):
            old = y[u, rows_of(s), :]
            new = min_plus(closed, jnp.concatenate(enc_right(old), 0), old)
            y[u, rows_of(s), :] = new
            ceil, floor = enc_right(new)
            enc_row[s % 2, u, 0:B, :] = ceil
            enc_row[s % 2, u, B : 2 * B, :] = floor

    start_b(0)

    @pl.when(here != 0)
    def _():
        take((16 - here) % 16)

    @pl.when(core == 0)
    def _():
        for d in range(1, 16):
            take_other(d)

    def square_and_take(i, block):
        block = min_plus_block(block)

        @pl.when(core == 1)
        def _():
            for d in range(3):
                take_other(1 + 3 * i + d)

        return block

    block = lax.fori_loop(0, 5, square_and_take, yp[0, 0].astype(F32) - 1.0)
    start_b(1)
    block = min_plus_block(block)

    for t in range(S):
        lanes = slice(t % 2 * B, (t % 2 + 1) * B)
        for s in range(S):
            y[t // 2, s * B : (s + 1) * B, lanes] = yp[t, s].astype(F32) - 1.0
        y[t // 2, S * B :, lanes] = yi[t].astype(F32) - 1.0

    for s in range(S - 1):
        panel(s, block)
        near = (s + 1) // 2
        update(s, s + 1, (near,))
        block = column(s + 1, s + 1)[...]
        rest = [(s + 1, (1 - near,))] + [(i, (0, 1)) for i in range(s + 2, 2 * S)]
        done = 0
        for q in range(6):
            until = -(-len(rest) * (q + 1) // 6)
            for i, which in rest[done:until]:
                update(s, i, which)
            block = min_plus_block(block)
            done = until
    panel(S - 1, block)
    for i in range(S, 2 * S, 4):
        update(S - 1, i, count=4)
    for t in range(S):
        x_ref[t] = y[t // 2, S * B :, t % 2 * B : (t % 2 + 1) * B].astype(BF16)

    for d in range(1, S):
        for copy in stage_b(d, (cx + d) % S, (cy + d) % S):
            copy.wait_recv()

    @pl.when(core == 0)
    def _():
        @pl.when(cy == 0)
        def _():
            for d in range(1, S):
                block_y(d).wait_send()

        for d in range(16):
            block_out(d, partner).wait_send()
        for d in range(S):
            cols_out(d, partner).wait_send()
        for d in range(1, S):
            cols_in((cz + d) % S, fi_send.at[d]).wait_send()
        for d in range(1, 16):
            ox, oz, _ = in_slab(d)
            block_in(ox, oz, pf_send.at[d], partner).wait_send()

    @pl.when(cy == 0)
    def _():
      for q in range(1, S):
          for copy in scatter(q):
              copy.wait_send()

    for d in range(1, S):
      for copy in stage_a(d, cx, cy):
          copy.wait_send()
    for d in range(1, S):
      for copy in stage_b(d, cx, cy):
          copy.wait_send()


def product_kernel(w, x_ref, r0, r1, o_hbm, o, o_sem):
    row, col = lax.axis_index("row"), lax.axis_index("col")
    wide = 2 * B
    parts = [pl.ds(j * wide, wide) for j in range(w.shape[1] // wide)]
    stores = [pltpu.make_async_copy(o.at[:, p], o_hbm.at[:, p], o_sem.at[j]) for j, p in enumerate(parts)]

    def right_operand(s, j):
        lanes = pl.ds(j % 2 * wide, wide)
        quarters = [(r0[q, s, :, lanes] if j < 2 else r1[s, q, :, lanes]) for q in range(S)]
        return jnp.concatenate(enc_right(jnp.concatenate(quarters, 0).astype(F32) - 1.0), 0)

    lefts = []
    for s in range(S):
        (f0, c0), (f1, c1) = enc_left(x_ref[s].astype(F32))
        lefts.append((f0, f1, c0, c1))
    for j, p in enumerate(parts):
        floors = ceils = None
        for s in range(S):
            right = right_operand(s, j)
            f0, f1, c0, c1 = (dot(left, right) for left in lefts[s])
            df, dc = jnp.maximum(f0, f1), jnp.maximum(c0, c1)
            floors = df if floors is None else jnp.maximum(floors, df)
            ceils = dc if ceils is None else jnp.maximum(ceils, dc)
        old = w[:, p]
        new = jnp.minimum(old.astype(F32), decode(floors, ceils, 2.0)).astype(jnp.int32)
        lag = lax.broadcasted_iota(jnp.int32, old.shape, 1) - lax.broadcasted_iota(jnp.int32, old.shape, 0)
        o[:, p] = jnp.where(lag == row * w.shape[0] - col * w.shape[1] - j * wide, 0, new)
        stores[j].start()
    for store in stores:
        store.wait()


def per_device(weights):
    dma = pltpu.SemaphoreType.DMA
    vmem = pl.BlockSpec(memory_space=pltpu.VMEM)
    rows, cols = weights.shape
    closed, r0, r1 = pl.pallas_call(
        gather_kernel,
        out_shape=(
            jax.ShapeDtypeStruct((S, rows, B), BF16),
            jax.ShapeDtypeStruct((S, S, 32, 512), BF16),
            jax.ShapeDtypeStruct((S, S, 32, 512), BF16),
        ),
        in_specs=[pl.BlockSpec(memory_space=pltpu.HBM)],
        out_specs=(vmem, vmem, vmem),
        scratch_shapes=[
            pltpu.VMEM((B, B), jnp.int32),
            pltpu.VMEM((B, cols), jnp.int32),
            pltpu.VMEM((rows, B), jnp.int32),
            pltpu.VMEM((S, 2, 32, 512), BF16),
            pltpu.VMEM((S, S, B, B), BF16),
            pltpu.VMEM((S, rows, B), BF16),
            pltpu.VMEM((2, 1024, 2 * B), F32),
            pltpu.VMEM((2, 2, 2 * B, 2 * B), BF16),
            dma((3,)), dma((S,)), dma, dma((16,)), dma((16,)), dma((16,)), dma((S,)), dma((S,)), dma((S,)),
            dma((S,)), dma, dma((S,)), dma,
            dma((S,)), dma((S,)), dma((S,)), dma((S,)), dma((S,)), dma((S,)), dma((S,)), dma((S,)),
        ],
        compiler_params=pltpu.CompilerParams(
            collective_id=0, has_side_effects=True, vmem_limit_bytes=24 * 2**20
        ),
        name="gather",
    )(pltpu.with_memory_space_constraint(weights, pltpu.HBM))
    return pl.pallas_call(
        product_kernel,
        out_shape=jax.ShapeDtypeStruct(weights.shape, jnp.int32),
        in_specs=[vmem] * 4,
        out_specs=pl.BlockSpec(memory_space=pltpu.HBM),
        scratch_shapes=[
            pltpu.VMEM((rows, cols), jnp.int32),
            dma((4,)),
        ],
        compiler_params=pltpu.CompilerParams(vmem_limit_bytes=32 * 2**20),
        name="product",
    )(weights, closed, r0, r1)


def solution(mesh):
    return jax.shard_map(
        per_device, mesh=mesh, in_specs=(P("row", "col"),), out_specs=P("row", "col"), check_vma=False
    )
```

```python
import math

import jax
import jax.numpy as jnp
from jax import lax
from jax.experimental import pallas as pl
from jax.experimental.pallas import tpu as pltpu
from jax.sharding import PartitionSpec as P

F32 = jnp.float32
BF16 = jnp.bfloat16
MESH = pl.DeviceIdType.MESH
ALPHA = 60.25
BETA = 6.2
SHIFT = 0.984
STEP = 2.0**-BETA
B = 128
S = 4


LOG = 1.0 / (BETA * math.log(2.0))
FLOOR = 2 * ALPHA / BETA + SHIFT


def encode(t):
    u = t * 0.5
    half = jnp.floor(u)
    return jnp.exp2(half * -BETA + ALPHA), u > half


def enc_right(t):
    e, odd = encode(t)
    return jnp.where(odd, e * STEP, e).astype(BF16), e.astype(BF16)


def split_left(t):
    e, odd = encode(t)
    odd_floor = jnp.where(odd, e, 0.0)
    return tuple(u.astype(BF16) for u in (odd_floor, jnp.where(odd, 0.0, e), odd_floor * STEP))


def enc_left(t):
    first = jnp.where(lax.broadcasted_iota(jnp.int32, t.shape, 1) < B // 2, 1.0, 0.0)
    pairs = []
    parts = split_left(t)
    for keep in (first.astype(BF16), (1.0 - first).astype(BF16)):
        of, ev, oc = (u * keep for u in parts)
        pairs.append((jnp.concatenate([of, ev], 1), jnp.concatenate([ev, oc], 1)))
    return pairs


def dot(left, right):
    return jnp.dot(left, right, preferred_element_type=F32)


def decode(floors, ceils, bias):
    low = jnp.floor(FLOOR - jnp.log(floors) * LOG)
    high = jnp.floor(FLOOR + bias - jnp.log(ceils) * LOG)
    return low + jnp.minimum(high, low + (1.0 + bias))


def min_plus(left, right, old):
    (f0, c0), (f1, c1) = left
    floors = jnp.maximum(dot(f0, right), dot(f1, right))
    ceils = jnp.maximum(dot(c0, right), dot(c1, right))
    return jnp.minimum(old, decode(floors, ceils, 1.0))


def min_plus_block(block):
    of, ev, oc = split_left(block)
    ceil, floor = enc_right(block)
    none = jnp.zeros((B // 2, B), BF16)
    first = jnp.concatenate([ceil[: B // 2], none, floor[: B // 2], none], 0)
    second = jnp.concatenate([none, ceil[B // 2 :], none, floor[B // 2 :]], 0)
    right = jnp.concatenate([first, second], 1)
    floors = dot(jnp.concatenate([of, ev], 1), right)
    ceils = dot(jnp.concatenate([ev, oc], 1), right)
    floors = jnp.maximum(floors[:, :B], floors[:, B:])
    ceils = jnp.maximum(ceils[:, :B], ceils[:, B:])
    return jnp.minimum(block, decode(floors, ceils, 1.0))


def remote(src, dst, send, recv, where):
    return pltpu.make_async_remote_copy(
        src_ref=src, dst_ref=dst, send_sem=send, recv_sem=recv, device_id=where, device_id_type=MESH
    )


def gather_kernel(
    w_hbm, x_ref, r0, r1, wp, wr, wc, rs, yp, yi, y, enc_row,
    w_sem, p1_send, p1_recv, p2_send, p2_recv, pf_send, yi_send, yi_recv, fi_send,
    s0_send, s0_recv, s1_send, s1_recv, a0_send, a0_recv, a1_send, a1_recv, b0_send, b0_recv, b1_send, b1_recv,
):
    row, col = lax.axis_index("row"), lax.axis_index("col")
    cx, cy = row // S, row % S
    cz, core = col // 2, col % 2
    block_owner = jnp.logical_and(cy == 0, core == 0)

    def at_x(x):
        return {"row": x * S + cy}

    def at_y(v):
        return {"row": cx * S + v}

    def in_slab(d):
        other = (cx * S + cz + d) % 16
        ox, oz = other // S, other % S
        return ox, oz, {"row": ox * S + cy, "col": oz * 2 + core}

    partner = {"col": cz * 2 + (1 - core)}

    barrier = pltpu.get_barrier_semaphore()

    def greet(where):
        pl.semaphore_signal(barrier, inc=1, device_id=where, device_id_type=MESH)

    for d in range(1, S):
        greet(at_y((cy + d) % S))
    for d in range(1, 16):
        greet(in_slab(d)[2])
    greet(partner)

    load_block = pltpu.make_async_copy(w_hbm.at[pl.ds(0, B), pl.ds(0, B)], wp, w_sem.at[0])
    load_rows = pltpu.make_async_copy(w_hbm.at[pl.ds(0, B)], wr, w_sem.at[1])
    load_cols = pltpu.make_async_copy(w_hbm.at[:, pl.ds(0, B)], wc, w_sem.at[2])

    @pl.when(block_owner)
    def _():
        load_block.start()

    @pl.when(cy == 0)
    def _():
        load_rows.start()

    @pl.when(core == 0)
    def _():
        load_cols.start()

    @pl.when(block_owner)
    def _():
        load_block.wait()
        yp[cz, cx] = wp[...].astype(BF16)

    pl.semaphore_wait(barrier, 19)

    def block_y(d):
        return remote(yp.at[cz, cx], yp.at[cz, cx], p1_send.at[d], p1_recv, at_y((cy + d) % S))

    def block_out(d, where):
        return remote(yp.at[cz, cx], yp.at[cz, cx], p2_send.at[d], p2_recv.at[cz * S + cx], where)

    def block_in(ox, oz, send, where):
        return remote(yp.at[oz, ox], yp.at[oz, ox], send, p2_recv.at[oz * S + ox], where)

    def cols_out(d, where):
        return remote(yi.at[cz], yi.at[cz], yi_send.at[d], yi_recv.at[cz], where)

    def cols_in(oz, send):
        return remote(yi.at[oz], yi.at[oz], send, yi_recv.at[oz], partner)

    def scatter(q):
        return (
            remote(rs.at[q, 0], r0.at[q, cx], s0_send.at[q], s0_recv, at_y(q)),
            remote(rs.at[q, 1], r1.at[cx, q], s1_send.at[q], s1_recv, at_y(q)),
        )

    def stage_a(d, x, v):
        return (
            remote(r0.at[cy, x], r0.at[cy, x], a0_send.at[d], a0_recv.at[x], at_x((cx + d) % S)),
            remote(r1.at[cx, v], r1.at[cx, v], a1_send.at[d], a1_recv.at[v], at_y((cy + d) % S)),
        )

    def stage_b(d, x, v):
        return (
            remote(r0.at[v], r0.at[v], b0_send.at[d], b0_recv.at[v], at_y((cy + d) % S)),
            remote(r1.at[x], r1.at[x], b1_send.at[d], b1_recv.at[x], at_x((cx + d) % S)),
        )

    def start_scatter():
        @pl.when(cy == 0)
        def _():
            for q in range(1, S):
                for copy in scatter(q):
                    copy.start()

    def start_a():
        @pl.when(cy != 0)
        def _():
            for copy in scatter(cy):
                copy.wait_recv()

        for d in range(1, S):
            for copy in stage_a(d, cx, cy):
                copy.start()

    def start_b(half):
        for d in range(1, S):
            stage_a(d, (cx + d) % S, (cy + d) % S)[half].wait_recv()
        for d in range(1, S):
            stage_b(d, cx, cy)[half].start()

    @pl.when(block_owner)
    def _():
        for d in range(1, S):
            block_y(d).start()

    @pl.when(core == 0)
    def _():
        load_cols.wait()
        yi[cz] = wc[...].astype(BF16)

    @pl.when(cy == 0)
    def _():
        load_rows.wait()
        for q in range(S):
            for h in range(2):
                rs[q, h] = wr[q * 32 : (q + 1) * 32, h * 512 : (h + 1) * 512].astype(BF16)
        r0[0, cx] = wr[0:32, 0:512].astype(BF16)
        r1[cx, 0] = wr[0:32, 512:1024].astype(BF16)

    @pl.when(core == 0)
    def _():
        for d in range(1, S):
            cols_out(d, {"col": (cz + d) % S * 2}).start()
        cols_out(0, partner).start()
        start_scatter()

        @pl.when(cy != 0)
        def _():
            block_y(0).wait_recv()

        for d in range(1, 16):
            block_out(d, in_slab(d)[2]).start()
        block_out(0, partner).start()
        start_a()
        for d in range(1, S):
            oz = (cz + d) % S
            cols_in(oz, yi_send.at[0]).wait_recv()
            cols_in(oz, fi_send.at[d]).start()

    @pl.when(core == 1)
    def _():
        start_scatter()
        start_a()
        for oz in range(S):
            cols_in(oz, yi_send.at[0]).wait_recv()
        block_in(cx, cz, p2_send.at[0], partner).wait_recv()

    here = cx * S + cz

    def take(d):
        ox, oz, _ = in_slab(d)
        block_in(ox, oz, p2_send.at[0], partner).wait_recv()

        @pl.when(core == 0)
        def _():
            block_in(ox, oz, pf_send.at[d], partner).start()

    def take_other(d):
        @pl.when((here + d) % 16 != 0)
        def _():
            take(d)

    def rows_of(i, count=1):
        return pl.ds(i * B, count * B)

    def column(s, i, count=1):
        return y.at[s // 2, rows_of(i, count), pl.ds(s % 2 * B, B)]

    def update(s, i, which=(0, 1), count=1):
        left = enc_left(column(s, i, count)[...])
        for u in which:
            y[u, rows_of(i, count), :] = min_plus(left, enc_row[s % 2, u], y[u, rows_of(i, count), :])

    def panel(s, block):
        column(s, s)[...] = block
        closed = enc_left(block)
        for u in range(2):
            old = y[u, rows_of(s), :]
            new = min_plus(closed, jnp.concatenate(enc_right(old), 0), old)
            y[u, rows_of(s), :] = new
            ceil, floor = enc_right(new)
            enc_row[s % 2, u, 0:B, :] = ceil
            enc_row[s % 2, u, B : 2 * B, :] = floor

    start_b(0)
    for t in range(S):
        y[t // 2, S * B :, t % 2 * B : (t % 2 + 1) * B] = yi[t].astype(F32) - 1.0

    @pl.when(here != 0)
    def _():
        take((16 - here) % 16)

    @pl.when(core == 0)
    def _():
        for d in range(1, 16):
            take_other(d)

    def square_and_take(i, block):
        block = min_plus_block(block)

        @pl.when(core == 1)
        def _():
            for d in range(3):
                take_other(1 + 3 * i + d)

        return block

    block = lax.fori_loop(0, 5, square_and_take, yp[0, 0].astype(F32) - 1.0)
    start_b(1)
    block = min_plus_block(block)

    for t in range(S):
        lanes = slice(t % 2 * B, (t % 2 + 1) * B)
        for s in range(S):
            y[t // 2, s * B : (s + 1) * B, lanes] = yp[t, s].astype(F32) - 1.0

    for s in range(S - 1):
        panel(s, block)
        near = (s + 1) // 2
        update(s, s + 1, (near,))
        block = column(s + 1, s + 1)[...]
        rest = [(s + 1, (1 - near,))] + [(i, (0, 1)) for i in range(s + 2, 2 * S)]
        done = 0
        for q in range(6):
            until = -(-len(rest) * (q + 1) // 6)
            for i, which in rest[done:until]:
                update(s, i, which)
            block = min_plus_block(block)
            done = until
    panel(S - 1, block)
    for i in range(S, 2 * S, 4):
        update(S - 1, i, count=4)
    for t in range(S):
        x_ref[t] = y[t // 2, S * B :, t % 2 * B : (t % 2 + 1) * B].astype(BF16)

    for d in range(1, S):
        for copy in stage_b(d, (cx + d) % S, (cy + d) % S):
            copy.wait_recv()

    @pl.when(core == 0)
    def _():
        @pl.when(cy == 0)
        def _():
            for d in range(1, S):
                block_y(d).wait_send()

        for d in range(16):
            block_out(d, partner).wait_send()
        for d in range(S):
            cols_out(d, partner).wait_send()
        for d in range(1, S):
            cols_in((cz + d) % S, fi_send.at[d]).wait_send()
        for d in range(1, 16):
            ox, oz, _ = in_slab(d)
            block_in(ox, oz, pf_send.at[d], partner).wait_send()

    @pl.when(cy == 0)
    def _():
      for q in range(1, S):
          for copy in scatter(q):
              copy.wait_send()

    for d in range(1, S):
      for copy in stage_a(d, cx, cy):
          copy.wait_send()
    for d in range(1, S):
      for copy in stage_b(d, cx, cy):
          copy.wait_send()


def product_kernel(w, x_ref, r0, r1, o_hbm, o, o_sem):
    row, col = lax.axis_index("row"), lax.axis_index("col")
    wide = 2 * B
    parts = [pl.ds(j * wide, wide) for j in range(w.shape[1] // wide)]
    stores = [pltpu.make_async_copy(o.at[:, p], o_hbm.at[:, p], o_sem.at[j]) for j, p in enumerate(parts)]

    def right_operand(s, j):
        lanes = pl.ds(j % 2 * wide, wide)
        quarters = [(r0[q, s, :, lanes] if j < 2 else r1[s, q, :, lanes]) for q in range(S)]
        return jnp.concatenate(enc_right(jnp.concatenate(quarters, 0).astype(F32) - 1.0), 0)

    lefts = []
    for s in range(S):
        (f0, c0), (f1, c1) = enc_left(x_ref[s].astype(F32))
        lefts.append((f0, f1, c0, c1))
    for j, p in enumerate(parts):
        floors = ceils = None
        for s in range(S):
            right = right_operand(s, j)
            f0, f1, c0, c1 = (dot(left, right) for left in lefts[s])
            df, dc = jnp.maximum(f0, f1), jnp.maximum(c0, c1)
            floors = df if floors is None else jnp.maximum(floors, df)
            ceils = dc if ceils is None else jnp.maximum(ceils, dc)
        old = w[:, p]
        new = jnp.minimum(old.astype(F32), decode(floors, ceils, 2.0)).astype(jnp.int32)
        lag = lax.broadcasted_iota(jnp.int32, old.shape, 1) - lax.broadcasted_iota(jnp.int32, old.shape, 0)
        o[:, p] = jnp.where(lag == row * w.shape[0] - col * w.shape[1] - j * wide, 0, new)
        stores[j].start()
    for store in stores:
        store.wait()


def per_device(weights):
    dma = pltpu.SemaphoreType.DMA
    vmem = pl.BlockSpec(memory_space=pltpu.VMEM)
    rows, cols = weights.shape
    closed, r0, r1 = pl.pallas_call(
        gather_kernel,
        out_shape=(
            jax.ShapeDtypeStruct((S, rows, B), BF16),
            jax.ShapeDtypeStruct((S, S, 32, 512), BF16),
            jax.ShapeDtypeStruct((S, S, 32, 512), BF16),
        ),
        in_specs=[pl.BlockSpec(memory_space=pltpu.HBM)],
        out_specs=(vmem, vmem, vmem),
        scratch_shapes=[
            pltpu.VMEM((B, B), jnp.int32),
            pltpu.VMEM((B, cols), jnp.int32),
            pltpu.VMEM((rows, B), jnp.int32),
            pltpu.VMEM((S, 2, 32, 512), BF16),
            pltpu.VMEM((S, S, B, B), BF16),
            pltpu.VMEM((S, rows, B), BF16),
            pltpu.VMEM((2, 1024, 2 * B), F32),
            pltpu.VMEM((2, 2, 2 * B, 2 * B), BF16),
            dma((3,)), dma((S,)), dma, dma((16,)), dma((16,)), dma((16,)), dma((S,)), dma((S,)), dma((S,)),
            dma((S,)), dma, dma((S,)), dma,
            dma((S,)), dma((S,)), dma((S,)), dma((S,)), dma((S,)), dma((S,)), dma((S,)), dma((S,)),
        ],
        compiler_params=pltpu.CompilerParams(
            collective_id=0, has_side_effects=True, vmem_limit_bytes=24 * 2**20
        ),
        name="gather",
    )(pltpu.with_memory_space_constraint(weights, pltpu.HBM))
    return pl.pallas_call(
        product_kernel,
        out_shape=jax.ShapeDtypeStruct(weights.shape, jnp.int32),
        in_specs=[vmem] * 4,
        out_specs=pl.BlockSpec(memory_space=pltpu.HBM),
        scratch_shapes=[
            pltpu.VMEM((rows, cols), jnp.int32),
            dma((4,)),
        ],
        compiler_params=pltpu.CompilerParams(vmem_limit_bytes=32 * 2**20),
        name="product",
    )(weights, closed, r0, r1)


def solution(mesh):
    return jax.shard_map(
        per_device, mesh=mesh, in_specs=(P("row", "col"),), out_specs=P("row", "col"), check_vma=False
    )
```
